256 devices in a mesh: boxes: 256 (over z, x, y, core).
Axes of the slice: x: 4, y: 4, z: 8, core: 2. Of those that a mesh axis runs over, the one named last changes fastest.
Arguments:
- conserved: float32 [256, 5, 16, 32, 128], P('boxes'), may hold values from -6 to 6
- volume_fraction: float32 [256, 16, 32, 128], P('boxes'), may hold values from 0.05 to 1
- cut_mask: int32 [256, 16, 32, 128], P('boxes'), may hold values 0 or 1
- merge_code: int32 [256, 16, 32, 128], P('boxes'), may hold values from 0 to 26
Outputs:
- redistributed: float32 [256, 5, 16, 32, 128], P('boxes')
The draws below stay inside these ranges and needn't reach their ends.
All inputs are finite; a program needn't handle non-finite values. No bound on the sum of `cut_mask` on one device may be relied on, other than what follows from the above.
Results may differ from the reference program's by a relative error of at most 0.0003.
Values sent between devices are 32-bit elements; how exact they have to be, the bound alone decides.
A program may use at most 64 MiB of HBM per device.

```python
import math
import jax
import jax.numpy as jnp
from jax import lax

FIELDS = 5
CX = 16
CY = 32
CZ = 128
NBY = 4
NBZ = 4
NBOXES = 256
NBX = 16
NX = 256
NY = 128
NZ = 512


def plant(array, stream_key, least, high):
    shape = array.shape
    spot = [jax.random.randint(jax.random.fold_in(stream_key, axis), (), 0, shape[axis]) for axis in range(len(shape))]
    array = array.at[tuple(spot)].set(least)
    longest = shape.index(max(shape))
    spot[longest] = (spot[longest] + 1) % shape[longest]
    return array.at[tuple(spot)].set(high)


def levels(key, dims, split, least, high):
    loudness, own = 1.0, jax.random.fold_in(key, 6)
    for dim, parts in split:
        steps = jnp.exp(jax.random.uniform(jax.random.fold_in(own, dim), (parts,), jnp.float32, least / len(split), high / len(split)))
        loudness = loudness * jnp.repeat(steps, dims[dim] // parts).reshape([-1 if axis == dim else 1 for axis in range(len(dims))])
    return loudness


def bell_draw(key, shape, width, limit, cuts=(), held_as=jnp.bfloat16):
    gain = levels(key, shape, cuts, -0.22, 0.18) if cuts else 1.0
    array = jax.random.normal(key, shape, jnp.float32) * width * gain
    return jnp.minimum(jnp.maximum(array, -limit), limit).astype(held_as)


def setup_inputs(seed: int = 0) -> dict:
    arg_keys = jax.random.split(jax.random.key(seed), 5)
    return {
        "conserved": bell_draw(arg_keys[0], (NBOXES, FIELDS, CX, CY, CZ), 1.0, 6.0, ((0, 256),), jnp.float32),
        "volume_fraction": jnp.clip(jnp.exp(math.log(1.0) - 2.9957323 * jax.random.uniform(arg_keys[1], (NBOXES, CX, CY, CZ), jnp.float32) ** levels(arg_keys[1], (NBOXES, CX, CY, CZ), ((0, 256),), -0.2, 0.2)), 0.05, 1.0),
        "cut_mask": plant((jax.random.randint(arg_keys[2], (NBOXES, CX, CY, CZ), 0, 2) < 1).astype(jnp.int32), jax.random.fold_in(arg_keys[2], 1), 0, 1),
        "merge_code": plant(jax.random.randint(arg_keys[3], (NBOXES, CX, CY, CZ), 0, 27), jax.random.fold_in(arg_keys[3], 1), 0, 26).astype(jnp.int32),
    }


OFFSETS = [(first, second, third) for first in (-1, 0, 1) for second in (-1, 0, 1) for third in (-1, 0, 1) if (first, second, third) != (0, 0, 0)]


def decode(code_field):
    sign_parts = (code_field // 9 - 1, (code_field // 3) % 3 - 1, code_field % 3 - 1)
    members = []
    for offset in OFFSETS:
        inside = jnp.ones(code_field.shape, jnp.bool_)
        for direction, component in zip(sign_parts, offset):
            if component != 0:
                inside = inside & (direction == component)
        members.append(inside)
    return members


def placed(values, offset):
    spread = [(0, 0)] * (values.ndim - 3) + [(1 + component, 1 - component) for component in offset]
    return jnp.pad(values, spread)


def count_members(members):
    running = placed(jnp.ones(members[0].shape, jnp.float32), (0, 0, 0))
    for offset, inside in zip(OFFSETS, members):
        running = running + placed(inside.astype(jnp.float32), offset)
    return running


def window(weighted, offset, interior):
    starts = [0] + [1 + component for component in offset]
    limits = [weighted.shape[0]] + [anchor + extent for anchor, extent in zip(starts[1:], interior)]
    return lax.slice(weighted, starts, limits)


def neighbour_average(weighted, members):
    interior = [extent - 2 for extent in weighted.shape[1:]]
    running = window(weighted, (0, 0, 0), interior)
    for offset, inside in zip(OFFSETS, members):
        running = running + jnp.where(inside[None], window(weighted, offset, interior), 0.0)
    return running[1:] / running[0:1]


def spread_back(average, members):
    running = placed(average, (0, 0, 0))
    for offset, inside in zip(OFFSETS, members):
        running = running + placed(jnp.where(inside[None], average, 0.0), offset)
    return running


def to_grid(boxed):
    channels = boxed.shape[1]
    shaped = boxed.reshape(NBX, NBY, NBZ, channels, CX, CY, CZ)
    return shaped.transpose(3, 0, 4, 1, 5, 2, 6).reshape(channels, NX, NY, NZ)


def from_grid(gridded):
    channels = gridded.shape[0]
    shaped = gridded.reshape(channels, NBX, CX, NBY, CY, NBZ, CZ)
    return shaped.transpose(1, 3, 5, 0, 2, 4, 6).reshape(NBOXES, channels, CX, CY, CZ)


def reference(conserved, volume_fraction, cut_mask, merge_code):
    fields = to_grid(conserved)
    fraction = to_grid(volume_fraction[:, None])[0]
    code_field = jnp.where(to_grid(cut_mask[:, None])[0] == 1, to_grid(merge_code[:, None])[0], 13)
    members = decode(code_field)
    counts = count_members(members)[1:-1, 1:-1, 1:-1]
    weight = fraction / counts
    weighted = jnp.concatenate([weight[None], weight[None] * fields], axis=0)
    weighted = jnp.pad(weighted, ((0, 0), (1, 1), (1, 1), (1, 1)))
    average = neighbour_average(weighted, members)
    gathered = spread_back(average, members)[:, 1:-1, 1:-1, 1:-1]
    return from_grid(gathered / counts[None])
```

```python
import functools

import jax
import jax.numpy as jnp
from jax import lax
from jax.experimental import pallas as pl
from jax.experimental.pallas import tpu as pltpu
from jax.sharding import PartitionSpec as P

NBY = 4
NBZ = 4
CX, CY, CZ = 16, 32, 128
MESH = pl.DeviceIdType.MESH

ROWS = 48
SLOT = 40
SIGNS = [(dx, dy) for dx in (-1, 0, 1) for dy in (-1, 0, 1)]


def lanes_of(shape):
    return lax.broadcasted_iota(jnp.int32, shape, len(shape) - 1)


def roll_lanes(a, by):
    return pltpu.roll(a, by % CZ, a.ndim - 1) if by % CZ else a


def roll_rows(a, by):
    return pltpu.roll(a, by % a.shape[0], 0) if by % a.shape[0] else a


def decode(code):
    xy = jnp.floor((code + 0.5) * (1.0 / 3.0))
    x = jnp.floor((code + 0.5) * (1.0 / 9.0))
    return xy, xy - 3.0 * x, code - 3.0 * xy


def towards(xy, y, dx, dy):
    if dy == 0:
        return xy >= 6.0 if dx == 1 else xy <= 2.0
    if dx == 0:
        return y == 1.0 + dy
    return xy == 3.0 * (dx + 1) + (dy + 1)


def moved(a, dx, dy):
    return roll_rows(roll_lanes(a, 2 * dx), dy)


def plane_spread(a, xy, y):
    up = towards(xy, y, 1, 0)
    down = towards(xy, y, -1, 0)

    def along_x(b):
        return b + moved(jnp.where(up, b, 0.0), 1, 0) + moved(jnp.where(down, b, 0.0), -1, 0)

    total = along_x(a)
    for dy in (-1, 1):
        total = total + moved(along_x(jnp.where(towards(xy, y, 0, dy), a, 0.0)), 0, dy)
    return total


def plane_gather(a, xy, y):
    left, right = towards(xy, y, 0, -1), towards(xy, y, 0, 1)

    def along_y(b):
        return b + jnp.where(right, moved(b, 0, -1), jnp.where(left, moved(b, 0, 1), 0.0))

    ahead, behind = along_y(moved(a, -1, 0)), along_y(moved(a, 1, 0))
    chosen = jnp.where(towards(xy, y, 1, 0), ahead, jnp.where(towards(xy, y, -1, 0), behind, 0.0))
    return along_y(a) + chosen


def in_all_slots(a, lane):
    return jnp.where(lane < SLOT, a, jnp.where(lane < 2 * SLOT, roll_lanes(a, SLOT), roll_lanes(a, 2 * SLOT)))


def rim_planes(own, ghost, lane):
    lower = lane % 2 == 1

    def signs(code):
        xy, y, z = decode(code)
        return xy, y, jnp.where(lower, z, 2.0 - z)

    near_own, far_own = signs(own[2]), signs(roll_lanes(own[2], -SLOT))
    near_ghost, far_ghost = signs(ghost[2]), signs(roll_lanes(ghost[2], -SLOT))
    one = jnp.ones(own[0].shape, jnp.float32)

    def spread_ones(plane, sign):
        xy, y, z = plane
        return plane_spread(one if sign == 0 else jnp.where(z == 1.0 + sign, 1.0, 0.0), xy, y)

    entering = spread_ones(near_ghost, 1)
    ghost_count = spread_ones(near_ghost, 0) + spread_ones(far_ghost, 1) + spread_ones(near_own, -1)
    own_count = spread_ones(near_own, 0) + entering + spread_ones(far_own, -1)
    last = lane >= 2 * SLOT

    def weighted(pack, count):
        w = in_all_slots(roll_lanes(pack[1], -2 * SLOT) / count, lane)
        return w * pack[0], w * jnp.where(last, 1.0, pack[1])

    ghost_w = weighted(ghost, ghost_count)
    own_w = weighted(own, own_count)
    xy, y, z = signs(in_all_slots(ghost[2], lane))
    sums = [plane_gather(a + b, xy, y) for a, b in zip(ghost_w, own_w)]
    volume = in_all_slots(roll_lanes(sums[1], -2 * SLOT), lane)
    deposits = [plane_spread(jnp.where(z == 2.0, s / volume, 0.0), xy, y) for s in sums]
    return entering, ghost_w, deposits


def kernel(
    sizes, u_hbm, vf_hbm, mask_hbm, code_hbm, out_hbm,
    uv, code, xy_v, y_v, z_v, ones_v, mask_raw, code_raw, y_send, y_recv, rim_own, z_recv, rim_calc,
    w_v, up_v, down_v, inv_v, avg_v, out_v,
    load_sem, x_send_sem, x_recv_sem, y_send_sem, y_recv_sem, d_send_sem, d_recv_sem, z_send_sem, z_recv_sem, out_sem,
):
    nbx, nby, nbz = sizes
    me = lax.axis_index("boxes")
    bx, by, bz = me // (nby * nbz), (me // nbz) % nby, me % nbz
    has_x = (bx > 0, bx < nbx - 1)
    has_y = (by > 0, by < nby - 1)
    has_z = (bz > 0, bz < nbz - 1)
    steps = (-1, 1)

    loads = [
        pltpu.make_async_copy(mask_hbm, mask_raw, load_sem.at[0]),
        pltpu.make_async_copy(code_hbm, code_raw, load_sem.at[1]),
        pltpu.make_async_copy(vf_hbm, uv.at[0, 1:17, 8:40], load_sem.at[2]),
        pltpu.make_async_copy(u_hbm, uv.at[1:6, 1:17, 8:40], load_sem.at[3]),
    ]
    for load in loads:
        load.start()

    barrier = pltpu.get_barrier_semaphore()
    greeted = 0
    for i in (0, 1):
        for cond, target in (
            (has_x[i], me + steps[i] * nby * nbz), (has_y[i], me + steps[i] * nbz), (has_z[i], me + steps[i]),
        ):
            @pl.when(cond)
            def _(target=target):
                pl.semaphore_signal(barrier, inc=1, device_id=(target,), device_id_type=MESH)
            greeted = greeted + cond.astype(jnp.int32)
        for j in (0, 1):
            cond = has_x[i] & has_y[j]
            target = me + steps[i] * nby * nbz + steps[j] * nbz

            @pl.when(cond)
            def _(target=target):
                pl.semaphore_signal(barrier, inc=1, device_id=(target,), device_id_type=MESH)
            greeted = greeted + cond.astype(jnp.int32)

    loads[0].wait()
    loads[1].wait()

    def mask_code(x, _):
        code[x + 2, 8:40, :] = jnp.where(mask_raw[x] == 1, code_raw[x], 13).astype(jnp.float32)
        return _

    lax.fori_loop(0, CX, mask_code, 0)
    loads[2].wait()
    loads[3].wait()

    def pack_y(x, _):
        for s, near, far in ((0, 8, 9), (1, 39, 38)):
            for q in range(6):
                y_send[s, x, q:q + 1, :] = uv[q, x + 1, near:near + 1, :]
            y_send[s, x, 6:7, :] = code[x + 2, near:near + 1, :]
            y_send[s, x, 7:8, :] = code[x + 2, far:far + 1, :]
        return _

    lax.fori_loop(0, CX, pack_y, 0)
    pl.semaphore_wait(barrier, greeted)

    def x_copies(i):
        target = (me + steps[i] * nby * nbz,)
        src_u, dst_u = (1, 17) if i == 0 else (16, 0)
        src_c, dst_c = (2, 18) if i == 0 else (16, 0)
        return [
            pltpu.make_async_remote_copy(
                src_ref=uv.at[:, src_u, 8:40], dst_ref=uv.at[:, dst_u, 8:40], send_sem=x_send_sem.at[i, 0],
                recv_sem=x_recv_sem.at[1 - i, 0], device_id=target, device_id_type=MESH),
            pltpu.make_async_remote_copy(
                src_ref=code.at[pl.ds(src_c, 2), 8:40], dst_ref=code.at[pl.ds(dst_c, 2), 8:40],
                send_sem=x_send_sem.at[i, 1], recv_sem=x_recv_sem.at[1 - i, 1], device_id=target, device_id_type=MESH),
        ]

    def y_copy(i):
        return pltpu.make_async_remote_copy(
            src_ref=y_send.at[i], dst_ref=y_recv.at[1 - i, 2:18], send_sem=y_send_sem.at[i],
            recv_sem=y_recv_sem.at[1 - i], device_id=(me + steps[i] * nbz,), device_id_type=MESH)

    def d_copy(i, j):
        src, dst = (0, 18) if i == 0 else (14, 0)
        return pltpu.make_async_remote_copy(
            src_ref=y_send.at[j, pl.ds(src, 2)], dst_ref=y_recv.at[1 - j, pl.ds(dst, 2)], send_sem=d_send_sem.at[i, j],
            recv_sem=d_recv_sem.at[1 - i, 1 - j], device_id=(me + steps[i] * nby * nbz + steps[j] * nbz,),
            device_id_type=MESH)

    def z_copy(i):
        return pltpu.make_async_remote_copy(
            src_ref=rim_own, dst_ref=z_recv.at[1 - i], send_sem=z_send_sem.at[i], recv_sem=z_recv_sem.at[1 - i],
            device_id=(me + steps[i],), device_id_type=MESH)

    for i in (0, 1):
        @pl.when(has_x[i])
        def _(i=i):
            for copy in x_copies(i):
                copy.start()
    for j in (0, 1):
        @pl.when(has_y[j])
        def _(j=j):
            y_copy(j).start()
        for i in (0, 1):
            @pl.when(has_x[i] & has_y[j])
            def _(i=i, j=j):
                d_copy(i, j).start()

    for i in (0, 1):
        @pl.when(jnp.logical_not(has_x[i]))
        def _(i=i):
            u_at, c_at = (0, 0) if i == 0 else (17, 18)
            for q in range(6):
                uv[q, u_at, 8:40, :] = jnp.zeros((CY, CZ), jnp.float32)
            for c in (0, 1):
                code[c_at + c, 8:40, :] = jnp.full((CY, CZ), 13.0, jnp.float32)

        def blank(first, count, j):
            row = lax.broadcasted_iota(jnp.int32, (8, CZ), 0)
            for x in range(count):
                y_recv[j, first + x] = jnp.where(row < 6, 0.0, 13.0)

        @pl.when(jnp.logical_not(has_y[i]))
        def _(i=i):
            blank(2, CX, i)

        for j in (0, 1):
            @pl.when(jnp.logical_not(has_x[i] & has_y[j]))
            def _(i=i, j=j):
                blank(0 if i == 0 else 18, 2, j)

    for s in (0, 1):
        @pl.when(has_y[s])
        def _(s=s):
            y_copy(1 - s).wait_recv()
        for i in (0, 1):
            @pl.when(has_x[i] & has_y[s])
            def _(i=i, s=s):
                d_copy(1 - i, 1 - s).wait_recv()
        @pl.when(has_x[s])
        def _(s=s):
            for copy in x_copies(1 - s):
                copy.wait_recv()

    def unpack_y(x, _):
        for s, near, far in ((0, 7, 6), (1, 40, 41)):
            code[x, near:near + 1, :] = y_recv[s, x, 6:7, :]
            code[x, far:far + 1, :] = y_recv[s, x, 7:8, :]
        return _

    def unpack_u(x, _):
        for s, near in ((0, 7), (1, 40)):
            for q in range(6):
                uv[q, x, near:near + 1, :] = y_recv[s, x + 1, q:q + 1, :]
        return _

    lax.fori_loop(0, 20, unpack_y, 0)
    lax.fori_loop(0, 18, unpack_u, 0)

    lane8 = lanes_of((8, CZ))

    def pack_rims(t, _):
        base = 6 + 8 * t
        blocks = [jnp.zeros((8, CZ), jnp.float32) for _ in range(3)]

        def place(block, value, slot, x):
            shift = slot * SLOT + 2 * x + 1
            hit = (lane8 // 2) == (slot * SLOT + 2 * x) // 2
            return jnp.where(hit, roll_lanes(value, shift), block)

        for x in range(20):
            near = code[x, pl.ds(base, 8), :]
            far = jnp.where(lane8 == CZ - 1, roll_lanes(near, 1), roll_lanes(near, -1))
            blocks[2] = place(blocks[2], near, 0, x)
            blocks[2] = place(blocks[2], far, 1, x)
            if 1 <= x <= 18:
                for q in range(5):
                    blocks[q // 3] = place(blocks[q // 3], uv[q + 1, x - 1, pl.ds(base, 8), :], q % 3, x)
                blocks[1] = place(blocks[1], uv[0, x - 1, pl.ds(base, 8), :], 2, x)
        for b in range(3):
            rim_own[b, pl.ds(pl.multiple_of(8 * t, 8), 8), :] = blocks[b]
        return _

    lax.fori_loop(0, 5, pack_rims, 0)
    for i in (0, 1):
        @pl.when(has_z[i])
        def _(i=i):
            z_copy(i).start()

        @pl.when(jnp.logical_not(has_z[i]))
        def _(i=i):
            for b in range(3):
                z_recv[i, b] = jnp.full((40, CZ), 13.0 if b == 2 else 0.0, jnp.float32)

    def signs(x, _):
        for t in range(5):
            rows = slice(6 + 8 * t, 14 + 8 * t)
            xy, y, z = decode(code[x, rows, :])
            xy_v[x, rows, :] = xy
            y_v[x, rows, :] = y
            z_v[x, rows, :] = z
            ones_v[x, rows, :] = jnp.where(z == 2.0, 257, jnp.where(z == 0.0, 65537, 1))
        return _

    lax.fori_loop(0, 20, signs, 0)

    for i in (0, 1):
        @pl.when(has_z[i])
        def _(i=i):
            z_copy(1 - i).wait_recv()

    lane40 = lanes_of((40, CZ))
    own = [rim_own[b] for b in range(3)]
    ghost = [jnp.where(lane40 % 2 == 1, roll_lanes(z_recv[0, b], 1), roll_lanes(z_recv[1, b], -1)) for b in range(3)]
    entering, ghost_w, deposits = rim_planes(own, ghost, lane40)
    for k, a in enumerate((entering, *ghost_w, *deposits)):
        rim_calc[k, 0:40, :] = a

    first, final = lane8 == 0, lane8 == CZ - 1

    def at_edges(k, slot, x, row):
        shift = CZ * 2 - (slot * SLOT + 2 * x + 1)
        return pltpu.roll(rim_calc[k, row:row + 8, :], lax.rem(shift, CZ), 1)

    def weights(x, _):
        for t in range(5):
            top = 7 + 8 * t
            rows = slice(top, top + 8)
            total = ones_v[x + 1, rows, :]
            for dx, dy in SIGNS:
                if (dx, dy) != (0, 0):
                    at = slice(top - dy, top - dy + 8)
                    hit = towards(xy_v[x + 1 - dx, at, :], y_v[x + 1 - dx, at, :], dx, dy)
                    total = total + jnp.where(hit, ones_v[x + 1 - dx, at, :], 0)
            here = (total & 255).astype(jnp.float32)
            up = ((total >> 8) & 255).astype(jnp.float32)
            down = (total >> 16).astype(jnp.float32)
            edge = at_edges(0, 0, x + 1, top - 6)
            count = here + jnp.where(first, edge, roll_lanes(up, 1)) + jnp.where(final, edge, roll_lanes(down, -1))
            inv = 1.0 / count
            inv_v[x, rows, :] = inv
            w = uv[0, x, rows, :] * inv
            for q in range(6):
                value = w if q == 0 else w * uv[q, x, rows, :]
                k, slot = (2, 2) if q == 0 else (1 + (q - 1) // 3, (q - 1) % 3)
                edge = at_edges(k, slot, x + 1, top - 6)
                w_v[q, x + 1, rows, :] = value
                up_v[q, x + 1, rows, :] = value + jnp.where(final, edge, roll_lanes(value, -1))
                down_v[q, x + 1, rows, :] = value + jnp.where(first, edge, roll_lanes(value, 1))
        return _

    lax.fori_loop(0, 18, weights, 0)

    def gather(x, _):
        for t in range(5):
            top = 7 + 8 * t
            rows = slice(top, top + 8)
            xy, y, z = xy_v[x + 1, rows, :], y_v[x + 1, rows, :], z_v[x + 1, rows, :]
            x_up, x_down = towards(xy, y, 1, 0), towards(xy, y, -1, 0)
            y_up, y_down = y == 2.0, y == 0.0
            z_up, z_down = z == 2.0, z == 0.0

            def total(q):
                def line(dx, dy):
                    at = slice(top + dy, top + dy + 8)
                    return jnp.where(z_up, up_v[q, x + 1 + dx, at, :], jnp.where(
                        z_down, down_v[q, x + 1 + dx, at, :], w_v[q, x + 1 + dx, at, :]))

                def plane(dx):
                    return line(dx, 0) + jnp.where(y_up, line(dx, 1), jnp.where(y_down, line(dx, -1), 0.0))

                return plane(0) + jnp.where(x_up, plane(1), jnp.where(x_down, plane(-1), 0.0))

            inv = 1.0 / total(0)
            for q in range(5):
                avg_v[q, x, rows, :] = total(q + 1) * inv
        return _

    lax.fori_loop(0, 18, gather, 0)

    def scatter(x, _):
        for t in range(4):
            top = 8 + 8 * t
            rows = slice(top, top + 8)
            here = [None] * 5
            up = [None] * 5
            down = [None] * 5
            for dx, dy in SIGNS:
                at = slice(top - dy, top - dy + 8)
                z = z_v[x + 2 - dx, at, :]
                z_up, z_down = z == 2.0, z == 0.0
                hit = None
                if (dx, dy) != (0, 0):
                    hit = towards(xy_v[x + 2 - dx, at, :], y_v[x + 2 - dx, at, :], dx, dy)
                    z_up, z_down = hit & z_up, hit & z_down
                for q in range(5):
                    a = avg_v[q, x + 1 - dx, at, :]
                    terms = (a if hit is None else jnp.where(hit, a, 0.0), jnp.where(z_up, a, 0.0), jnp.where(z_down, a, 0.0))
                    here[q], up[q], down[q] = (
                        new if old is None else old + new for old, new in zip((here[q], up[q], down[q]), terms))
            inv = inv_v[x + 1, rows, :]
            for q in range(5):
                edge = at_edges(3 + q // 3, q % 3, x + 2, top - 6)
                total = here[q] + jnp.where(first, edge, roll_lanes(up[q], 1)) + jnp.where(
                    final, edge, roll_lanes(down[q], -1))
                out_v[q, x, 8 * t:8 * t + 8, :] = total * inv
        return _

    lax.fori_loop(0, CX, scatter, 0)
    out_copy = pltpu.make_async_copy(out_v, out_hbm, out_sem)
    out_copy.start()

    for i in (0, 1):
        @pl.when(has_x[i])
        def _(i=i):
            for copy in x_copies(i):
                copy.wait_send()

        @pl.when(has_y[i])
        def _(i=i):
            y_copy(i).wait_send()

        for j in (0, 1):
            @pl.when(has_x[i] & has_y[j])
            def _(i=i, j=j):
                d_copy(i, j).wait_send()

        @pl.when(has_z[i])
        def _(i=i):
            z_copy(i).wait_send()
    out_copy.wait()


def solution(mesh, nby=NBY, nbz=NBZ):
    nbx = mesh.shape["boxes"] // (nby * nbz)
    f32 = jnp.float32

    def per_device(conserved, volume_fraction, cut_mask, merge_code):
        dma = pltpu.SemaphoreType.DMA
        out = pl.pallas_call(
            functools.partial(kernel, (nbx, nby, nbz)),
            out_shape=jax.ShapeDtypeStruct((5, CX, CY, CZ), f32),
            in_specs=[pl.BlockSpec(memory_space=pl.ANY)] * 4,
            out_specs=pl.BlockSpec(memory_space=pl.ANY),
            scratch_shapes=[
                pltpu.VMEM((6, 18, ROWS, CZ), f32),
                pltpu.VMEM((20, ROWS, CZ), f32),
                pltpu.VMEM((20, ROWS, CZ), f32),
                pltpu.VMEM((20, ROWS, CZ), f32),
                pltpu.VMEM((20, ROWS, CZ), f32),
                pltpu.VMEM((20, ROWS, CZ), jnp.int32),
                pltpu.VMEM((CX, CY, CZ), jnp.int32),
                pltpu.VMEM((CX, CY, CZ), jnp.int32),
                pltpu.VMEM((2, CX, 8, CZ), f32),
                pltpu.VMEM((2, 20, 8, CZ), f32),
                pltpu.VMEM((3, 40, CZ), f32),
                pltpu.VMEM((2, 3, 40, CZ), f32),
                pltpu.VMEM((5, ROWS, CZ), f32),
                pltpu.VMEM((6, 20, ROWS, CZ), f32),
                pltpu.VMEM((6, 20, ROWS, CZ), f32),
                pltpu.VMEM((6, 20, ROWS, CZ), f32),
                pltpu.VMEM((18, ROWS, CZ), f32),
                pltpu.VMEM((5, 18, ROWS, CZ), f32),
                pltpu.VMEM((5, CX, CY, CZ), f32),
                dma((4,)), dma((2, 2)), dma((2, 2)), dma((2,)), dma((2,)), dma((2, 2)), dma((2, 2)), dma((2,)), dma((2,)),
                dma,
            ],
            compiler_params=pltpu.CompilerParams(
                collective_id=0, has_side_effects=True, vmem_limit_bytes=60 * 1024 * 1024
            ),
        )(conserved[0], volume_fraction[0], cut_mask[0], merge_code[0])
        return out[None]

    return jax.shard_map(
        per_device,
        mesh=mesh,
        in_specs=(
            P("boxes", None, None, None, None),
            P("boxes", None, None, None),
            P("boxes", None, None, None),
            P("boxes", None, None, None),
        ),
        out_specs=P("boxes", None, None, None, None),
        check_vma=False,
    )
```

```python
import functools

import jax
import jax.numpy as jnp
from jax import lax
from jax.experimental import pallas as pl
from jax.experimental.pallas import tpu as pltpu
from jax.sharding import PartitionSpec as P

NBY = 4
NBZ = 4
CX, CY, CZ = 16, 32, 128
MESH = pl.DeviceIdType.MESH

ROWS = 48
SLOT = 40
SIGNS = [(dx, dy) for dx in (-1, 0, 1) for dy in (-1, 0, 1)]


def lanes_of(shape):
    return lax.broadcasted_iota(jnp.int32, shape, len(shape) - 1)


def roll_lanes(a, by):
    return pltpu.roll(a, by % CZ, a.ndim - 1) if by % CZ else a


def roll_rows(a, by):
    return pltpu.roll(a, by % a.shape[0], 0) if by % a.shape[0] else a


def decode(code):
    xy = jnp.floor((code + 0.5) * (1.0 / 3.0))
    x = jnp.floor((code + 0.5) * (1.0 / 9.0))
    return xy, xy - 3.0 * x, code - 3.0 * xy


def towards(xy, y, dx, dy):
    if dy == 0:
        return xy >= 6.0 if dx == 1 else xy <= 2.0
    if dx == 0:
        return y == 1.0 + dy
    return xy == 3.0 * (dx + 1) + (dy + 1)


def moved(a, dx, dy):
    return roll_rows(roll_lanes(a, 2 * dx), dy)


def plane_spread(a, xy, y):
    up = towards(xy, y, 1, 0)
    down = towards(xy, y, -1, 0)

    def along_x(b):
        return b + moved(jnp.where(up, b, 0.0), 1, 0) + moved(jnp.where(down, b, 0.0), -1, 0)

    total = along_x(a)
    for dy in (-1, 1):
        total = total + moved(along_x(jnp.where(towards(xy, y, 0, dy), a, 0.0)), 0, dy)
    return total


def plane_gather(a, xy, y):
    left, right = towards(xy, y, 0, -1), towards(xy, y, 0, 1)

    def along_y(b):
        return b + jnp.where(right, moved(b, 0, -1), jnp.where(left, moved(b, 0, 1), 0.0))

    ahead, behind = along_y(moved(a, -1, 0)), along_y(moved(a, 1, 0))
    chosen = jnp.where(towards(xy, y, 1, 0), ahead, jnp.where(towards(xy, y, -1, 0), behind, 0.0))
    return along_y(a) + chosen


def in_all_slots(a, lane):
    return jnp.where(lane < SLOT, a, jnp.where(lane < 2 * SLOT, roll_lanes(a, SLOT), roll_lanes(a, 2 * SLOT)))


def rim_planes(own, ghost, lane):
    lower = lane % 2 == 1

    def signs(code):
        xy, y, z = decode(code)
        return xy, y, jnp.where(lower, z, 2.0 - z)

    near_own, far_own = signs(own[2]), signs(roll_lanes(own[2], -SLOT))
    near_ghost, far_ghost = signs(ghost[2]), signs(roll_lanes(ghost[2], -SLOT))
    one = jnp.ones(own[0].shape, jnp.float32)

    def spread_ones(plane, sign):
        xy, y, z = plane
        return plane_spread(one if sign == 0 else jnp.where(z == 1.0 + sign, 1.0, 0.0), xy, y)

    entering = spread_ones(near_ghost, 1)
    ghost_count = spread_ones(near_ghost, 0) + spread_ones(far_ghost, 1) + spread_ones(near_own, -1)
    own_count = spread_ones(near_own, 0) + entering + spread_ones(far_own, -1)
    last = lane >= 2 * SLOT

    def weighted(pack, count):
        w = in_all_slots(roll_lanes(pack[1], -2 * SLOT) / count, lane)
        return w * pack[0], w * jnp.where(last, 1.0, pack[1])

    ghost_w = weighted(ghost, ghost_count)
    own_w = weighted(own, own_count)
    xy, y, z = signs(in_all_slots(ghost[2], lane))
    sums = [plane_gather(a + b, xy, y) for a, b in zip(ghost_w, own_w)]
    volume = in_all_slots(roll_lanes(sums[1], -2 * SLOT), lane)
    deposits = [plane_spread(jnp.where(z == 2.0, s / volume, 0.0), xy, y) for s in sums]
    return entering, ghost_w, deposits


TILES = 5


def kernel(
    sizes, u_hbm, vf_hbm, mask_hbm, code_hbm, out_ref,
    uv, code, xy_v, y_v, z_v, xz_v, yz_v, ones_v, total_v, mask_raw, code_raw, y_send, y_recv, rim_own, rim_ghost, rim_x,
    rim_ghost_x, rim_calc, w_v, up_v, down_v, inv_v, avg_v,
    load_sem, x_send_sem, x_recv_sem, y_send_sem, y_recv_sem, d_send_sem, d_recv_sem, z_send_sem, z_recv_sem,
    yz_send_sem, yz_recv_sem, zx_send_sem, zx_recv_sem,
):
    nbx, nby, nbz = sizes
    me = lax.axis_index("boxes")
    bx, by, bz = me // (nby * nbz), (me // nbz) % nby, me % nbz
    has_x = (bx > 0, bx < nbx - 1)
    has_y = (by > 0, by < nby - 1)
    has_z = (bz > 0, bz < nbz - 1)
    has_yz = [[has_y[j] & has_z[i] for i in (0, 1)] for j in (0, 1)]
    steps = (-1, 1)
    x_step, y_step = nby * nbz, nbz

    def when(cond):
        return pl.when(cond)

    barrier = pltpu.get_barrier_semaphore()
    greeted = 0
    for i in (0, 1):
        met = [(has_x[i], steps[i] * x_step), (has_y[i], steps[i] * y_step), (has_z[i], steps[i])]
        met += [(has_yz[j][i], steps[j] * y_step + steps[i]) for j in (0, 1)]
        for cond, step in met:
            @when(cond)
            def _(step=step):
                pl.semaphore_signal(barrier, inc=1, device_id=(me + step,), device_id_type=MESH)
            greeted = greeted + cond.astype(jnp.int32)

    loads = [
        pltpu.make_async_copy(mask_hbm, mask_raw, load_sem.at[0]),
        pltpu.make_async_copy(code_hbm, code_raw, load_sem.at[1]),
        pltpu.make_async_copy(vf_hbm, uv.at[0, 2:18, 8:40], load_sem.at[2]),
        pltpu.make_async_copy(u_hbm, uv.at[1:6, 2:18, 8:40], load_sem.at[3]),
    ]
    for load in loads:
        load.start()

    def remote(src, dst, send, recv, step):
        return pltpu.make_async_remote_copy(
            src_ref=src, dst_ref=dst, send_sem=send, recv_sem=recv, device_id=(me + step,), device_id_type=MESH)

    def x_copies(i):
        src_u, dst_u = (2, 18) if i == 0 else (17, 1)
        src_c, dst_c = (2, 18) if i == 0 else (16, 0)
        return [
            remote(uv.at[:, src_u, 8:40], uv.at[:, dst_u, 8:40], x_send_sem.at[i, 0], x_recv_sem.at[1 - i, 0],
                   steps[i] * x_step),
            remote(code.at[pl.ds(src_c, 2), 8:40], code.at[pl.ds(dst_c, 2), 8:40], x_send_sem.at[i, 1],
                   x_recv_sem.at[1 - i, 1], steps[i] * x_step),
        ]

    def d_copy(i):
        src, dst = (2, 18) if i == 0 else (16, 0)
        return remote(y_recv.at[:, pl.ds(src, 2)], y_recv.at[:, pl.ds(dst, 2)], d_send_sem.at[i], d_recv_sem.at[1 - i],
                      steps[i] * x_step)

    rim_src, rim_dst = (8, 32), (40, 0)

    def y_copies(i, which=None):
        return [
            remote(y_send.at[i], y_recv.at[1 - i, 2:18], y_send_sem.at[i, 0], y_recv_sem.at[1 - i, 0], steps[i] * y_step),
        ] * (which != 1) + [
            remote(rim_own.at[:, pl.ds(rim_src[i], 8)], rim_own.at[:, pl.ds(rim_dst[i], 8)], y_send_sem.at[i, 1],
                   y_recv_sem.at[1 - i, 1], steps[i] * y_step),
        ] * (which != 0)

    def z_copy(i):
        return remote(rim_own.at[:, 8:40], rim_ghost.at[1 - i, :, 8:40], z_send_sem.at[i], z_recv_sem.at[1 - i], steps[i])

    def yz_copy(j, i):
        return remote(
            rim_own.at[:, pl.ds(rim_src[j], 8)], rim_ghost.at[1 - i, :, pl.ds(rim_dst[j], 8)], yz_send_sem.at[j, i],
            yz_recv_sem.at[1 - j, 1 - i], steps[j] * y_step + steps[i])

    def zx_copy(i):
        return remote(rim_x, rim_ghost_x.at[1 - i], zx_send_sem.at[i], zx_recv_sem.at[1 - i], steps[i])

    loads[0].wait()
    loads[1].wait()

    def write_signs(X, base):
        rows = pl.ds(base, 8)
        c = code[X, rows, :]
        xy, y, z = decode(c)
        xy_v[X, rows, :] = xy
        y_v[X, rows, :] = y
        z_v[X, rows, :] = z
        xz_v[X, rows, :] = xy - y + z
        yz_v[X, rows, :] = 3.0 * y + z
        ones_v[X, rows, :] = jnp.where(z == 2.0, 257, jnp.where(z == 0.0, 65537, 1))

    def own_codes(x, _):
        code[x + 2, 8:40, :] = jnp.where(mask_raw[x] == 1, code_raw[x], 13).astype(jnp.float32)
        return _

    lax.fori_loop(0, CX, own_codes, 0)
    loads[2].wait()
    loads[3].wait()

    def pack_y(x, _):
        for s, near, far in ((0, 8, 9), (1, 39, 38)):
            for q in range(6):
                y_send[s, x, q:q + 1, :] = uv[q, x + 2, near:near + 1, :]
            y_send[s, x, 6:7, :] = code[x + 2, near:near + 1, :]
            y_send[s, x, 7:8, :] = code[x + 2, far:far + 1, :]
        return _

    lax.fori_loop(0, CX, pack_y, 0)
    lane8 = lanes_of((8, CZ))

    def pack_rims(rim, slabs, base):
        blocks = [jnp.zeros((8, CZ), jnp.float32) for _ in range(3)]

        def place(b, value, slot, X):
            lane = slot * SLOT + 2 * X
            blocks[b] = jnp.where(lane8 // 2 == lane // 2, roll_lanes(value, lane + 1), blocks[b])

        for X in slabs:
            near = code[X, pl.ds(base, 8), :]
            place(2, near, 0, X)
            place(2, jnp.where(lane8 == CZ - 1, roll_lanes(near, 1), roll_lanes(near, -1)), 1, X)
            if 1 <= X <= 18:
                for q in range(5):
                    place(q // 3, uv[q + 1, X, pl.ds(base, 8), :], q % 3, X)
                place(1, uv[0, X, pl.ds(base, 8), :], 2, X)
        for b in range(3):
            rim[b, pl.ds(base, 8), :] = blocks[b]

    def pack_own_rims(t, _):
        pack_rims(rim_own, range(2, 18), pl.multiple_of(8 + 8 * t, 8))
        return _

    lax.fori_loop(0, 4, pack_own_rims, 0)
    pl.semaphore_wait(barrier, greeted)

    for i in (0, 1):
        @when(has_y[i])
        def _(i=i):
            for copy in y_copies(i):
                copy.start()

        @when(has_z[i])
        def _(i=i):
            z_copy(i).start()

        for j in (0, 1):
            @when(has_yz[j][i])
            def _(i=i, j=j):
                yz_copy(j, i).start()
    for i in (0, 1):
        @when(has_x[i])
        def _(i=i):
            for copy in x_copies(i):
                copy.start()

    tile_row = lax.broadcasted_iota(jnp.int32, (8, CZ), 0)

    def blank_rim(rim, first, rows):
        for b in range(3):
            rim[b, first:first + rows, :] = jnp.full((rows, CZ), 13.0 if b == 2 else 0.0, jnp.float32)

    for s in (0, 1):
        @when(jnp.logical_not(has_y[s]))
        def _(s=s):
            blank_rim(rim_own, 0 if s == 0 else 40, 8)
            for X in range(2, 18):
                y_recv[s, X] = jnp.where(tile_row < 6, 0.0, 13.0)

        @when(jnp.logical_not(has_z[s]))
        def _(s=s):
            blank_rim(rim_ghost.at[s], 8, 32)
            blank_rim(rim_ghost_x.at[s], 0, ROWS)

        for j in (0, 1):
            @when(jnp.logical_not(has_yz[j][s]))
            def _(s=s, j=j):
                blank_rim(rim_ghost.at[s], 0 if j == 0 else 40, 8)

        @when(jnp.logical_not(has_x[s]))
        def _(s=s):
            u_at, c_at = (1, 0) if s == 0 else (18, 18)
            for q in range(6):
                uv[q, u_at, 8:40, :] = jnp.zeros((CY, CZ), jnp.float32)
            for c in (0, 1):
                code[c_at + c, 8:40, :] = jnp.full((CY, CZ), 13.0, jnp.float32)
                for j in (0, 1):
                    y_recv[j, c_at + c] = jnp.where(tile_row < 6, 0.0, 13.0)

    def count(X, tiles):
        for t in tiles:
            top = 7 + 8 * t
            total = ones_v[X, top:top + 8, :]
            for dx, dy in SIGNS:
                if (dx, dy) != (0, 0):
                    at = slice(top - dy, top - dy + 8)
                    signs = (y_v if dx == 0 else xy_v)[X - dx, at, :]
                    total = total + jnp.where(towards(signs, signs, dx, dy), ones_v[X - dx, at, :], 0)
            total_v[X, top:top + 8, :] = total

    first, final = lane8 == 0, lane8 == CZ - 1

    def at_edges(k, slot, X, top):
        shift = CZ * 2 - (slot * SLOT + 2 * X + 1)
        return pltpu.roll(rim_calc[k, pl.ds(top, 8), :], lax.rem(shift, CZ), 1)

    def weigh(X):
        for t in range(TILES):
            top = 7 + 8 * t
            rows = slice(top, top + 8)
            total = total_v[X, rows, :]
            here = (total & 255).astype(jnp.float32)
            up = ((total >> 8) & 255).astype(jnp.float32)
            down = (total >> 16).astype(jnp.float32)
            edge = at_edges(0, 0, X, top)
            inv = 1.0 / (here + jnp.where(first, edge, roll_lanes(up, 1)) + jnp.where(final, edge, roll_lanes(down, -1)))
            inv_v[X, rows, :] = inv
            w = uv[0, X, rows, :] * inv
            for q in range(6):
                value = w if q == 0 else w * uv[q, X, rows, :]
                k, slot = (2, 2) if q == 0 else (1 + (q - 1) // 3, (q - 1) % 3)
                edge = at_edges(k, slot, X, top)
                w_v[q, X, rows, :] = value
                up_v[q, X, rows, :] = value + jnp.where(final, edge, roll_lanes(value, -1))
                down_v[q, X, rows, :] = value + jnp.where(first, edge, roll_lanes(value, 1))

    def gather(start, slabs, t):
        top = 7 + 8 * t
        rows = pl.ds(top, 8)

        def step(X, behind, here, ahead):
            targets = []
            for dx, use in ((1, behind), (0, here), (-1, ahead)):
                if use is not None:
                    y, z = y_v[X - dx, rows, :], z_v[X - dx, rows, :]
                    along = None if dx == 0 else towards(xy_v[X - dx, rows, :], None, dx, 0)
                    targets.append((dx, along, y == 2.0, y == 0.0, z == 2.0, z == 0.0))
            new = {dx: [] for dx, *_ in targets}
            for q in range(6):
                lines = [[ref[q, X, pl.ds(top + dy, 8), :] for ref in (up_v, down_v, w_v)] for dy in (-1, 0, 1)]
                for dx, along, y_up, y_down, z_up, z_down in targets:
                    low, mid, high = (jnp.where(z_up, a, jnp.where(z_down, b, c)) for a, b, c in lines)
                    plane = mid + jnp.where(y_up, high, jnp.where(y_down, low, 0.0))
                    if along is not None:
                        plane = jnp.where(along, plane, 0.0)
                    old = {1: behind, 0: here, -1: ahead}[dx][q]
                    new[dx].append(plane if old is None else old + plane)
            return new

        none = [None] * 6
        one = step(start - 1, None, None, none)[-1]
        both = step(start, None, one, none)

        def walk(X, sums):
            new = step(X, list(sums[:6]), list(sums[6:]), none)
            inv = 1.0 / new[1][0]
            for q in range(5):
                avg_v[q, X - 1, rows, :] = new[1][q + 1] * inv
            return (*new[0], *new[-1])

        lax.fori_loop(start + 1, start + slabs + 1, walk, (*both[0], *both[-1]))

    def scatter(X):
        for t in range(4):
            top = 8 + 8 * t
            here, up, down = [None] * 5, [None] * 5, [None] * 5
            for dx, dy in SIGNS:
                at = slice(top - dy, top - dy + 8)
                if (dx, dy) == (0, 0):
                    z = z_v[X, at, :]
                    hit, z_up, z_down = None, z == 2.0, z == 0.0
                else:
                    signs = (y_v if dx == 0 else xy_v)[X - dx, at, :]
                    hit = towards(signs, signs, dx, dy)
                    z = (code if dx * dy else yz_v if dx == 0 else xz_v)[X - dx, at, :]
                    full = 9 * (dx + 1) + 3 * (dy + 1) if dx * dy else 3 * (dx + dy + 1)
                    z_up, z_down = z == full + 2.0, z == full + 0.0
                for q in range(5):
                    a = avg_v[q, X - dx, at, :]
                    terms = (a if hit is None else jnp.where(hit, a, 0.0), jnp.where(z_up, a, 0.0), jnp.where(z_down, a, 0.0))
                    here[q], up[q], down[q] = (
                        new if old is None else old + new for old, new in zip((here[q], up[q], down[q]), terms))
            inv = inv_v[X, top:top + 8, :]
            for q in range(5):
                edge = at_edges(3 + q // 3, q % 3, X, top)
                total = here[q] + jnp.where(first, edge, roll_lanes(up[q], 1)) + jnp.where(
                    final, edge, roll_lanes(down[q], -1))
                out_ref[q, X - 2, 8 * t:8 * t + 8, :] = total * inv

    def loop(lo, hi, body):
        def step(k, _):
            body(k)
            return _

        lax.fori_loop(lo, hi, step, 0)

    def both_ends(k, low, high):
        return k + low + (k // 2) * (high - low - 2)

    def unpack_y(X, fields):
        for s, near, far in ((0, 7, 6), (1, 40, 41)):
            code[X, near:near + 1, :] = y_recv[s, X, 6:7, :]
            code[X, far:far + 1, :] = y_recv[s, X, 7:8, :]
            if fields:
                for q in range(6):
                    uv[q, X, near:near + 1, :] = y_recv[s, X, q:q + 1, :]

    lane = lanes_of((ROWS, CZ))

    def planes(own, from_lower, from_upper):
        ghost = [jnp.where(lane % 2 == 1, roll_lanes(a, 1), roll_lanes(b, -1)) for a, b in zip(from_lower, from_upper)]
        entering, ghost_w, deposits = rim_planes(own, ghost, lane)
        for k, a in enumerate((entering, *ghost_w, *deposits)):
            rim_calc[k] = a

    def own_signs(X):
        for t in range(4):
            write_signs(X, 8 + 8 * t)

    loop(2, 18, own_signs)
    loop(3, 17, lambda X: count(X, (1, 2, 3)))

    for s in (0, 1):
        @when(has_y[s])
        def _(s=s):
            y_copies(1 - s, 0)[0].wait_recv()
    for i in (0, 1):
        @when(has_x[i])
        def _(i=i):
            d_copy(i).start()

    def y_ghosts(X):
        unpack_y(X, True)

    loop(2, 18, y_ghosts)

    def ghost_signs(X):
        write_signs(X, 0)
        write_signs(X, 40)

    loop(2, 18, ghost_signs)
    loop(3, 17, lambda X: count(X, (0, 4)))

    for s in (0, 1):
        @when(has_y[s])
        def _(s=s):
            y_copies(1 - s, 1)[0].wait_recv()

        @when(has_z[s])
        def _(s=s):
            z_copy(1 - s).wait_recv()

        for j in (0, 1):
            @when(has_yz[j][s])
            def _(s=s, j=j):
                yz_copy(1 - j, 1 - s).wait_recv()
    planes([rim_own[b] for b in range(3)], [rim_ghost[0, b] for b in range(3)], [rim_ghost[1, b] for b in range(3)])

    loop(3, 17, weigh)
    loop(0, TILES, lambda t: gather(3, 14, t))

    for s in (0, 1):
        @when(has_x[s])
        def _(s=s):
            for copy in x_copies(1 - s):
                copy.wait_recv()
            d_copy(1 - s).wait_recv()

    loop(0, 2, lambda k: unpack_y(1 + 17 * k, True))
    loop(0, 2, lambda k: unpack_y(19 * k, False))
    loop(0, TILES, lambda t: pack_rims(rim_x, (0, 1, 18, 19), 6 + 8 * t))
    for i in (0, 1):
        @when(has_z[i])
        def _(i=i):
            zx_copy(i).start()

    def end_signs(k):
        for t in range(6):
            write_signs(both_ends(k, 0, 18), 8 * t)

    loop(0, 4, end_signs)
    loop(0, 4, lambda k: count(both_ends(k, 1, 17), range(TILES)))
    loop(4, 16, scatter)
    for s in (0, 1):
        @when(has_z[s])
        def _(s=s):
            zx_copy(1 - s).wait_recv()
    place = lane % SLOT
    at_x = (place < 4) | (place >= 36)

    def with_x(rim, rim_of_x):
        return [jnp.where(at_x, rim_of_x[b], rim[b]) for b in range(3)]

    planes(with_x(rim_own, rim_x), *(with_x(rim_ghost.at[s], rim_ghost_x.at[s]) for s in (0, 1)))
    loop(0, 4, lambda k: weigh(both_ends(k, 1, 17)))
    loop(0, 2 * TILES, lambda k: gather(1 + 15 * (k // TILES), 3, k % TILES))
    loop(0, 4, lambda k: scatter(both_ends(k, 2, 16)))

    for i in (0, 1):
        @when(has_x[i])
        def _(i=i):
            for copy in (*x_copies(i), d_copy(i)):
                copy.wait_send()

        @when(has_y[i])
        def _(i=i):
            for copy in y_copies(i):
                copy.wait_send()

        @when(has_z[i])
        def _(i=i):
            z_copy(i).wait_send()
            zx_copy(i).wait_send()

        for j in (0, 1):
            @when(has_yz[j][i])
            def _(i=i, j=j):
                yz_copy(j, i).wait_send()


def solution(mesh, nby=NBY, nbz=NBZ):
    nbx = mesh.shape["boxes"] // (nby * nbz)
    f32 = jnp.float32

    def per_device(*args):
        dma = pltpu.SemaphoreType.DMA
        extended = pltpu.VMEM((21, ROWS, CZ), f32)
        values = pltpu.VMEM((6, 21, ROWS, CZ), f32)
        out = pl.pallas_call(
            functools.partial(kernel, (nbx, nby, nbz)),
            out_shape=jax.ShapeDtypeStruct((5, CX, CY, CZ), f32),
            in_specs=[pl.BlockSpec(memory_space=pltpu.HBM)] * 4,
            out_specs=pl.BlockSpec(memory_space=pltpu.VMEM),
            scratch_shapes=[
                values,
                extended, extended, extended, extended, extended, extended,
                pltpu.VMEM((21, ROWS, CZ), jnp.int32),
                pltpu.VMEM((21, ROWS, CZ), jnp.int32),
                pltpu.VMEM((CX, CY, CZ), jnp.int32),
                pltpu.VMEM((CX, CY, CZ), jnp.int32),
                pltpu.VMEM((2, CX, 8, CZ), f32),
                pltpu.VMEM((2, 20, 8, CZ), f32),
                pltpu.VMEM((3, ROWS, CZ), f32),
                pltpu.VMEM((2, 3, ROWS, CZ), f32),
                pltpu.VMEM((3, ROWS, CZ), f32),
                pltpu.VMEM((2, 3, ROWS, CZ), f32),
                pltpu.VMEM((5, ROWS, CZ), f32),
                values, values, values,
                extended,
                values,
                dma((4,)), dma((2, 2)), dma((2, 2)), dma((2, 2)), dma((2, 2)), dma((2,)), dma((2,)), dma((2,)), dma((2,)),
                dma((2, 2)), dma((2, 2)), dma((2,)), dma((2,)),
            ],
            compiler_params=pltpu.CompilerParams(
                collective_id=0, has_side_effects=True, vmem_limit_bytes=30 * 1024 * 1024
            ),
        )(*(pltpu.with_memory_space_constraint(a[0], pltpu.HBM) for a in args))
        return out[None]

    return jax.shard_map(
        per_device,
        mesh=mesh,
        in_specs=(
            P("boxes", None, None, None, None),
            P("boxes", None, None, None),
            P("boxes", None, None, None),
            P("boxes", None, None, None),
        ),
        out_specs=P("boxes", None, None, None, None),
        check_vma=False,
    )
```

```python
import functools

import jax
import jax.numpy as jnp
from jax import lax
from jax.experimental import pallas as pl
from jax.experimental.pallas import tpu as pltpu
from jax.sharding import PartitionSpec as P

NBY = 4
NBZ = 4
CX, CY, CZ = 16, 32, 128
MESH = pl.DeviceIdType.MESH

ROWS = 48
SLOT = 40
SIGNS = [(dx, dy) for dx in (-1, 0, 1) for dy in (-1, 0, 1)]


def lanes_of(shape):
    return lax.broadcasted_iota(jnp.int32, shape, len(shape) - 1)


def roll_lanes(a, by):
    return pltpu.roll(a, by % CZ, a.ndim - 1) if by % CZ else a


def roll_rows(a, by):
    return pltpu.roll(a, by % a.shape[0], 0) if by % a.shape[0] else a


def decode(code):
    xy = jnp.floor((code + 0.5) * (1.0 / 3.0))
    x = jnp.floor((code + 0.5) * (1.0 / 9.0))
    return xy, xy - 3.0 * x, code - 3.0 * xy


def towards(xy, y, dx, dy):
    if dy == 0:
        return xy >= 6.0 if dx == 1 else xy <= 2.0
    if dx == 0:
        return y == 1.0 + dy
    return xy == 3.0 * (dx + 1) + (dy + 1)


def moved(a, dx, dy):
    return roll_rows(roll_lanes(a, 2 * dx), dy)


def plane_spread(a, xy, y):
    up = towards(xy, y, 1, 0)
    down = towards(xy, y, -1, 0)

    def along_x(b):
        return b + moved(jnp.where(up, b, 0.0), 1, 0) + moved(jnp.where(down, b, 0.0), -1, 0)

    total = along_x(a)
    for dy in (-1, 1):
        total = total + moved(along_x(jnp.where(towards(xy, y, 0, dy), a, 0.0)), 0, dy)
    return total


def plane_gather(a, xy, y):
    left, right = towards(xy, y, 0, -1), towards(xy, y, 0, 1)

    def along_y(b):
        return b + jnp.where(right, moved(b, 0, -1), jnp.where(left, moved(b, 0, 1), 0.0))

    ahead, behind = along_y(moved(a, -1, 0)), along_y(moved(a, 1, 0))
    chosen = jnp.where(towards(xy, y, 1, 0), ahead, jnp.where(towards(xy, y, -1, 0), behind, 0.0))
    return along_y(a) + chosen


def in_all_slots(a, lane):
    return jnp.where(lane < SLOT, a, jnp.where(lane < 2 * SLOT, roll_lanes(a, SLOT), roll_lanes(a, 2 * SLOT)))


def rim_planes(own, ghost, lane):
    lower = lane % 2 == 1

    def signs(code):
        xy, y, z = decode(code)
        return xy, y, jnp.where(lower, z, 2.0 - z)

    near_own, far_own = signs(own[2]), signs(roll_lanes(own[2], -SLOT))
    near_ghost, far_ghost = signs(ghost[2]), signs(roll_lanes(ghost[2], -SLOT))
    one = jnp.ones(own[0].shape, jnp.float32)

    def spread_ones(plane, sign):
        xy, y, z = plane
        return plane_spread(one if sign == 0 else jnp.where(z == 1.0 + sign, 1.0, 0.0), xy, y)

    entering = spread_ones(near_ghost, 1)
    ghost_count = spread_ones(near_ghost, 0) + spread_ones(far_ghost, 1) + spread_ones(near_own, -1)
    own_count = spread_ones(near_own, 0) + entering + spread_ones(far_own, -1)
    last = lane >= 2 * SLOT

    def weighted(pack, count):
        w = in_all_slots(roll_lanes(pack[1], -2 * SLOT) / count, lane)
        return w * pack[0], w * jnp.where(last, 1.0, pack[1])

    ghost_w = weighted(ghost, ghost_count)
    own_w = weighted(own, own_count)
    xy, y, z = signs(in_all_slots(ghost[2], lane))
    sums = [plane_gather(a + b, xy, y) for a, b in zip(ghost_w, own_w)]
    volume = in_all_slots(roll_lanes(sums[1], -2 * SLOT), lane)
    deposits = [plane_spread(jnp.where(z == 2.0, s / volume, 0.0), xy, y) for s in sums]
    return entering, ghost_w, deposits


TILES = 5


def kernel(
    sizes, u_hbm, vf_hbm, mask_hbm, code_hbm, out_ref,
    uv, code, xy_v, y_v, z_v, xz_v, yz_v, ones_v, total_v, mask_raw, code_raw, y_send, y_recv, rim_own, rim_ghost, edge_send,
    edge_own, edge_ghost, rim_calc, w_v, up_v, down_v, inv_v, avg_v,
    load_sem, x_send_sem, x_recv_sem, y_send_sem, y_recv_sem, d_send_sem, d_recv_sem, z_send_sem, z_recv_sem,
    yz_send_sem, yz_recv_sem, ex_send_sem, ex_recv_sem, ey_send_sem, ey_recv_sem, ez_send_sem, ez_recv_sem,
):
    nbx, nby, nbz = sizes
    me = lax.axis_index("boxes")
    bx, by, bz = me // (nby * nbz), (me // nbz) % nby, me % nbz
    has_x = (bx > 0, bx < nbx - 1)
    has_y = (by > 0, by < nby - 1)
    has_z = (bz > 0, bz < nbz - 1)
    has_yz = [[has_y[j] & has_z[i] for i in (0, 1)] for j in (0, 1)]
    steps = (-1, 1)
    x_step, y_step = nby * nbz, nbz

    def when(cond):
        return pl.when(cond)

    barrier = pltpu.get_barrier_semaphore()
    greeted = 0
    for i in (0, 1):
        met = [(has_x[i], steps[i] * x_step), (has_y[i], steps[i] * y_step), (has_z[i], steps[i])]
        met += [(has_yz[j][i], steps[j] * y_step + steps[i]) for j in (0, 1)]
        for cond, step in met:
            @when(cond)
            def _(step=step):
                pl.semaphore_signal(barrier, inc=1, device_id=(me + step,), device_id_type=MESH)
            greeted = greeted + cond.astype(jnp.int32)

    loads = [
        pltpu.make_async_copy(mask_hbm, mask_raw, load_sem.at[0]),
        pltpu.make_async_copy(code_hbm, code_raw, load_sem.at[1]),
        pltpu.make_async_copy(vf_hbm, uv.at[0, 2:18, 8:40], load_sem.at[2]),
        pltpu.make_async_copy(u_hbm, uv.at[1:6, 2:18, 8:40], load_sem.at[3]),
    ]
    for load in loads:
        load.start()

    def remote(src, dst, send, recv, step):
        return pltpu.make_async_remote_copy(
            src_ref=src, dst_ref=dst, send_sem=send, recv_sem=recv, device_id=(me + step,), device_id_type=MESH)

    def x_copies(i):
        src_u, dst_u = (2, 18) if i == 0 else (17, 1)
        src_c, dst_c = (2, 18) if i == 0 else (16, 0)
        return [
            remote(uv.at[:, src_u, 8:40], uv.at[:, dst_u, 8:40], x_send_sem.at[i, 0], x_recv_sem.at[1 - i, 0],
                   steps[i] * x_step),
            remote(code.at[pl.ds(src_c, 2), 8:40], code.at[pl.ds(dst_c, 2), 8:40], x_send_sem.at[i, 1],
                   x_recv_sem.at[1 - i, 1], steps[i] * x_step),
        ]

    def d_copy(i):
        src, dst = (2, 18) if i == 0 else (16, 0)
        return remote(y_recv.at[:, pl.ds(src, 2)], y_recv.at[:, pl.ds(dst, 2)], d_send_sem.at[i], d_recv_sem.at[1 - i],
                      steps[i] * x_step)

    rim_src, rim_dst = (8, 32), (40, 0)

    def y_copies(i, which=None):
        return [
            remote(y_send.at[i], y_recv.at[1 - i, 2:18], y_send_sem.at[i, 0], y_recv_sem.at[1 - i, 0], steps[i] * y_step),
        ] * (which != 1) + [
            remote(rim_own.at[0:3, pl.ds(rim_src[i], 8)], rim_own.at[0:3, pl.ds(rim_dst[i], 8)], y_send_sem.at[i, 1],
                   y_recv_sem.at[1 - i, 1], steps[i] * y_step),
        ] * (which != 0)

    def z_copy(i):
        return remote(rim_own.at[0:3, 8:40], rim_ghost.at[1 - i, 0:3, 8:40], z_send_sem.at[i], z_recv_sem.at[1 - i], steps[i])

    def yz_copy(j, i):
        return remote(
            rim_own.at[0:3, pl.ds(rim_src[j], 8)], rim_ghost.at[1 - i, 0:3, pl.ds(rim_dst[j], 8)], yz_send_sem.at[j, i],
            yz_recv_sem.at[1 - j, 1 - i], steps[j] * y_step + steps[i])

    def ex_copy(i):
        return remote(edge_send, edge_own.at[1 - i, 8:40], ex_send_sem.at[i], ex_recv_sem.at[1 - i], steps[i] * x_step)

    def ey_copy(i):
        return remote(edge_own.at[:, pl.ds(rim_src[i], 8)], edge_own.at[:, pl.ds(rim_dst[i], 8)], ey_send_sem.at[i],
                      ey_recv_sem.at[1 - i], steps[i] * y_step)

    def ez_copy(i, part):
        rows = pl.ds((8, 0, 40)[part], (32, 8, 8)[part])
        return remote(edge_own.at[:, rows], edge_ghost.at[1 - i, :, rows], ez_send_sem.at[i, part],
                      ez_recv_sem.at[1 - i, part], steps[i])

    loads[0].wait()
    loads[1].wait()

    def write_signs(X, base):
        rows = pl.ds(base, 8)
        c = code[X, rows, :]
        xy, y, z = decode(c)
        xy_v[X, rows, :] = xy
        y_v[X, rows, :] = y
        z_v[X, rows, :] = z
        xz_v[X, rows, :] = xy - y + z
        yz_v[X, rows, :] = 3.0 * y + z
        ones_v[X, rows, :] = jnp.where(z == 2.0, 257, jnp.where(z == 0.0, 65537, 1))

    def own_codes(x, _):
        code[x + 2, 8:40, :] = jnp.where(mask_raw[x] == 1, code_raw[x], 13).astype(jnp.float32)
        return _

    lax.fori_loop(0, CX, own_codes, 0)
    loads[2].wait()
    loads[3].wait()

    def pack_y(x, _):
        for s, near, far in ((0, 8, 9), (1, 39, 38)):
            for q in range(6):
                y_send[s, x, q:q + 1, :] = uv[q, x + 2, near:near + 1, :]
            y_send[s, x, 6:7, :] = code[x + 2, near:near + 1, :]
            y_send[s, x, 7:8, :] = code[x + 2, far:far + 1, :]
        return _

    lax.fori_loop(0, CX, pack_y, 0)
    lane8 = lanes_of((8, CZ))

    def pack_rims(rim, slabs, base):
        blocks = [jnp.zeros((8, CZ), jnp.float32) for _ in range(3)]

        def place(b, value, slot, X):
            lane = slot * SLOT + 2 * X
            blocks[b] = jnp.where(lane8 // 2 == lane // 2, roll_lanes(value, lane + 1), blocks[b])

        for X in slabs:
            near = code[X, pl.ds(base, 8), :]
            place(2, near, 0, X)
            place(2, jnp.where(lane8 == CZ - 1, roll_lanes(near, 1), roll_lanes(near, -1)), 1, X)
            if 1 <= X <= 18:
                for q in range(5):
                    place(q // 3, uv[q + 1, X, pl.ds(base, 8), :], q % 3, X)
                place(1, uv[0, X, pl.ds(base, 8), :], 2, X)
        for b in range(3):
            rim[b, pl.ds(base, 8), :] = blocks[b]

    def pack_own_rims(t, _):
        pack_rims(rim_own, range(2, 18), pl.multiple_of(8 + 8 * t, 8))
        return _

    lax.fori_loop(0, 4, pack_own_rims, 0)

    lane32 = lanes_of((CY, CZ))
    kept = ((lane32 % SLOT) // 4 == 1) | ((lane32 % SLOT) // 4 == 8)
    compact = jnp.zeros((CY, CZ), jnp.float32)
    for b in range(3):
        compact = compact + roll_lanes(jnp.where(kept & (lane32 < (2 if b == 2 else 3) * SLOT), rim_own[b, 8:40, :], 0.0), 8 * b)
    edge_send[...] = compact
    pl.semaphore_wait(barrier, greeted)

    for i in (0, 1):
        @when(has_z[i])
        def _(i=i):
            z_copy(i).start()
    for i in (0, 1):
        @when(has_x[i])
        def _(i=i):
            ex_copy(i).start()
    for i in (0, 1):
        @when(has_y[i])
        def _(i=i):
            for copy in y_copies(i):
                copy.start()

        for j in (0, 1):
            @when(has_yz[j][i])
            def _(i=i, j=j):
                yz_copy(j, i).start()
    for i in (0, 1):
        @when(has_x[i])
        def _(i=i):
            for copy in x_copies(i):
                copy.start()

    tile_row = lax.broadcasted_iota(jnp.int32, (8, CZ), 0)

    def blank_rim(rim, first, rows):
        for b in range(3):
            rim[b, first:first + rows, :] = jnp.full((rows, CZ), 13.0 if b == 2 else 0.0, jnp.float32)

    def blank_edge(rows):
        spot = lanes_of((rows, CZ)) - 16
        is_code = (spot >= 0) & (spot < 2 * SLOT) & (((spot % SLOT) // 4 == 1) | ((spot % SLOT) // 4 == 8))
        return jnp.where(is_code, 13.0, 0.0)

    for s in (0, 1):
        @when(jnp.logical_not(has_y[s]))
        def _(s=s):
            for side in (0, 1):
                edge_own[side, 40 * s:40 * s + 8, :] = blank_edge(8)
            blank_rim(rim_own, 0 if s == 0 else 40, 8)
            for X in range(2, 18):
                y_recv[s, X] = jnp.where(tile_row < 6, 0.0, 13.0)

        @when(jnp.logical_not(has_z[s]))
        def _(s=s):
            blank_rim(rim_ghost.at[s], 8, 32)
            for side in (0, 1):
                edge_ghost[s, side] = blank_edge(ROWS)

        for j in (0, 1):
            @when(jnp.logical_not(has_yz[j][s]))
            def _(s=s, j=j):
                blank_rim(rim_ghost.at[s], 0 if j == 0 else 40, 8)

        @when(jnp.logical_not(has_x[s]))
        def _(s=s):
            u_at, c_at = (1, 0) if s == 0 else (18, 18)
            edge_own[s, 8:40, :] = blank_edge(CY)
            for q in range(6):
                uv[q, u_at, 8:40, :] = jnp.zeros((CY, CZ), jnp.float32)
            for c in (0, 1):
                code[c_at + c, 8:40, :] = jnp.full((CY, CZ), 13.0, jnp.float32)
                for j in (0, 1):
                    y_recv[j, c_at + c] = jnp.where(tile_row < 6, 0.0, 13.0)

    def count(X, tiles):
        for t in tiles:
            top = 7 + 8 * t
            total = ones_v[X, top:top + 8, :]
            for dx, dy in SIGNS:
                if (dx, dy) != (0, 0):
                    at = slice(top - dy, top - dy + 8)
                    signs = (y_v if dx == 0 else xy_v)[X - dx, at, :]
                    total = total + jnp.where(towards(signs, signs, dx, dy), ones_v[X - dx, at, :], 0)
            total_v[X, top:top + 8, :] = total

    first, final = lane8 == 0, lane8 == CZ - 1

    def at_edges(k, slot, X, top):
        shift = CZ * 2 - (slot * SLOT + 2 * X + 1)
        return pltpu.roll(rim_calc[k, pl.ds(top, 8), :], lax.rem(shift, CZ), 1)

    def weigh(X, tiles=range(TILES)):
        for t in tiles:
            top = 7 + 8 * t
            rows = pl.ds(top, 8)
            total = total_v[X, rows, :]
            here = (total & 255).astype(jnp.float32)
            up = ((total >> 8) & 255).astype(jnp.float32)
            down = (total >> 16).astype(jnp.float32)
            edge = at_edges(0, 0, X, top)
            inv = 1.0 / (here + jnp.where(first, edge, roll_lanes(up, 1)) + jnp.where(final, edge, roll_lanes(down, -1)))
            inv_v[X, rows, :] = inv
            w = uv[0, X, rows, :] * inv
            for q in range(6):
                value = w if q == 0 else w * uv[q, X, rows, :]
                k, slot = (2, 2) if q == 0 else (1 + (q - 1) // 3, (q - 1) % 3)
                edge = at_edges(k, slot, X, top)
                w_v[q, X, rows, :] = value
                up_v[q, X, pl.ds(top + 8, 8), :] = value + jnp.where(final, edge, roll_lanes(value, -1))
                down_v[q, X, pl.ds(top + 16, 8), :] = value + jnp.where(first, edge, roll_lanes(value, 1))

    def gather(start, slabs, t):
        top = 7 + 8 * t
        rows = pl.ds(top, 8)

        def step(X, behind, here, ahead):
            targets = []
            for dx, use in ((1, behind), (0, here), (-1, ahead)):
                if use is not None:
                    y, z = y_v[X - dx, rows, :], z_v[X - dx, rows, :]
                    along = None if dx == 0 else towards(xy_v[X - dx, rows, :], None, dx, 0)
                    targets.append((dx, along, y == 2.0, y == 0.0, z == 2.0, z == 0.0))
            new = {dx: [] for dx, *_ in targets}
            for q in range(6):
                lines = [[ref[q, X, pl.ds(top + dy + shift, 8), :] for ref, shift in ((up_v, 8), (down_v, 16), (w_v, 0))] for dy in (-1, 0, 1)]
                for dx, along, y_up, y_down, z_up, z_down in targets:
                    low, mid, high = (jnp.where(z_up, a, jnp.where(z_down, b, c)) for a, b, c in lines)
                    plane = mid + jnp.where(y_up, high, jnp.where(y_down, low, 0.0))
                    if along is not None:
                        plane = jnp.where(along, plane, 0.0)
                    old = {1: behind, 0: here, -1: ahead}[dx][q]
                    new[dx].append(plane if old is None else old + plane)
            return new

        none = [None] * 6
        one = step(start - 1, None, None, none)[-1]
        both = step(start, None, one, none)

        def walk(X, sums):
            new = step(X, list(sums[:6]), list(sums[6:]), none)
            inv = 1.0 / new[1][0]
            for q in range(5):
                avg_v[q, X - 1, rows, :] = new[1][q + 1] * inv
            return (*new[0], *new[-1])

        lax.fori_loop(start + 1, start + slabs + 1, walk, (*both[0], *both[-1]))

    def scatter(X, tiles=range(4)):
        for t in tiles:
            top = 8 + 8 * t
            here, up, down = [None] * 5, [None] * 5, [None] * 5
            for dx, dy in SIGNS:
                at = pl.ds(top - dy, 8)
                if (dx, dy) == (0, 0):
                    z = z_v[X, at, :]
                    hit, z_up, z_down = None, z == 2.0, z == 0.0
                else:
                    signs = (y_v if dx == 0 else xy_v)[X - dx, at, :]
                    hit = towards(signs, signs, dx, dy)
                    z = (code if dx * dy else yz_v if dx == 0 else xz_v)[X - dx, at, :]
                    full = 9 * (dx + 1) + 3 * (dy + 1) if dx * dy else 3 * (dx + dy + 1)
                    z_up, z_down = z == full + 2.0, z == full + 0.0
                for q in range(5):
                    a = avg_v[q, X - dx, at, :]
                    terms = (a if hit is None else jnp.where(hit, a, 0.0), jnp.where(z_up, a, 0.0), jnp.where(z_down, a, 0.0))
                    here[q], up[q], down[q] = (
                        new if old is None else old + new for old, new in zip((here[q], up[q], down[q]), terms))
            inv = inv_v[X, pl.ds(top, 8), :]
            for q in range(5):
                edge = at_edges(3 + q // 3, q % 3, X, top)
                total = here[q] + jnp.where(first, edge, roll_lanes(up[q], 1)) + jnp.where(
                    final, edge, roll_lanes(down[q], -1))
                out_ref[q, X - 2, pl.ds(8 * t if isinstance(t, int) else pl.multiple_of(8 * t, 8), 8), :] = total * inv

    def loop(lo, hi, body):
        def step(k, _):
            body(k)
            return _

        lax.fori_loop(lo, hi, step, 0)

    def both_ends(k, low, high):
        return k + low + (k // 2) * (high - low - 2)

    def unpack_y(X, fields):
        for s, near, far in ((0, 7, 6), (1, 40, 41)):
            code[X, near:near + 1, :] = y_recv[s, X, 6:7, :]
            code[X, far:far + 1, :] = y_recv[s, X, 7:8, :]
            if fields:
                for q in range(6):
                    uv[q, X, near:near + 1, :] = y_recv[s, X, q:q + 1, :]

    lane = lanes_of((ROWS, CZ))

    def planes(own, from_lower, from_upper, inner=False):
        lane = lanes_of(own[0].shape)
        ghost = [jnp.where(lane % 2 == 1, roll_lanes(a, 1), roll_lanes(b, -1)) for a, b in zip(from_lower, from_upper)]
        entering, ghost_w, deposits = rim_planes(own, ghost, lane)
        for k, a in enumerate((entering, *ghost_w) if inner else (entering, *ghost_w, *deposits)):
            rim_calc[k, 8 if inner else 0:40 if inner else ROWS, :] = a

    def own_signs(X):
        for t in range(4):
            write_signs(X, 8 + 8 * t)

    loop(2, 18, own_signs)
    loop(3, 17, lambda X: count(X, (1, 2, 3)))

    for s in (0, 1):
        @when(has_z[s])
        def _(s=s):
            z_copy(1 - s).wait_recv()
    planes(*([rim[b, 8:40, :] for b in range(3)] for rim in (rim_own, rim_ghost.at[0], rim_ghost.at[1])), inner=True)
    loop(3, 17, lambda X: weigh(X, (1, 2, 3)))
    gather(3, 14, 2)

    for s in (0, 1):
        @when(has_y[s])
        def _(s=s):
            y_copies(1 - s, 0)[0].wait_recv()
    for i in (0, 1):
        @when(has_x[i])
        def _(i=i):
            d_copy(i).start()

    def y_ghosts(X):
        unpack_y(X, True)

    loop(2, 18, y_ghosts)

    def ghost_signs(X):
        write_signs(X, 0)
        write_signs(X, 40)

    loop(2, 18, ghost_signs)
    loop(3, 17, lambda X: count(X, (0, 4)))

    for s in (0, 1):
        @when(has_x[s])
        def _(s=s):
            ex_copy(1 - s).wait_recv()
    for i in (0, 1):
        @when(has_y[i])
        def _(i=i):
            ey_copy(i).start()

        @when(has_z[i])
        def _(i=i):
            ez_copy(i, 0).start()

    for s in (0, 1):
        @when(has_y[s])
        def _(s=s):
            y_copies(1 - s, 1)[0].wait_recv()

        for j in (0, 1):
            @when(has_yz[j][s])
            def _(s=s, j=j):
                yz_copy(1 - j, 1 - s).wait_recv()
    planes([rim_own[b] for b in range(3)], [rim_ghost[0, b] for b in range(3)], [rim_ghost[1, b] for b in range(3)])

    loop(3, 17, lambda X: weigh(X, (0, 4)))
    for s in (0, 1):
        @when(has_y[s])
        def _(s=s):
            ey_copy(1 - s).wait_recv()
    for i in (0, 1):
        @when(has_z[i])
        def _(i=i):
            ez_copy(i, 1).start()
            ez_copy(i, 2).start()
    loop(0, TILES - 1, lambda k: gather(3, 14, k + k // 2))
    loop(4, 16, scatter)

    for s in (0, 1):
        @when(has_z[s])
        def _(s=s):
            for part in range(3):
                ez_copy(1 - s, part).wait_recv()
    place = lane % SLOT
    at_x = (place < 4) | (place >= 36)

    def with_x(rim, edge):
        low, high = edge[0], edge[1]
        return [
            jnp.where(at_x, jnp.where(place < 4, roll_lanes(low, -(32 + 8 * b)), roll_lanes(high, 32 - 8 * b)), rim[b])
            for b in range(3)
        ]

    planes(with_x(rim_own, edge_own), *(with_x(rim_ghost.at[s], edge_ghost.at[s]) for s in (0, 1)))

    for s in (0, 1):
        @when(has_x[s])
        def _(s=s):
            for copy in x_copies(1 - s):
                copy.wait_recv()
            d_copy(1 - s).wait_recv()

    loop(0, 2, lambda k: unpack_y(1 + 17 * k, True))
    loop(0, 2, lambda k: unpack_y(19 * k, False))

    def end_signs(k):
        for t in range(6):
            write_signs(both_ends(k, 0, 18), 8 * t)

    loop(0, 4, end_signs)
    loop(0, 4, lambda k: count(both_ends(k, 1, 17), range(TILES)))
    loop(0, 4, lambda k: weigh(both_ends(k, 1, 17)))
    loop(0, 2 * TILES, lambda k: gather(1 + 15 * (k // TILES), 3, k % TILES))
    loop(0, 4, lambda k: scatter(both_ends(k, 2, 16)))

    for i in (0, 1):
        @when(has_x[i])
        def _(i=i):
            for copy in (*x_copies(i), d_copy(i), ex_copy(i)):
                copy.wait_send()

        @when(has_y[i])
        def _(i=i):
            for copy in (*y_copies(i), ey_copy(i)):
                copy.wait_send()

        @when(has_z[i])
        def _(i=i):
            for copy in (z_copy(i), *(ez_copy(i, part) for part in range(3))):
                copy.wait_send()

        for j in (0, 1):
            @when(has_yz[j][i])
            def _(i=i, j=j):
                yz_copy(j, i).wait_send()


def solution(mesh, nby=NBY, nbz=NBZ):
    nbx = mesh.shape["boxes"] // (nby * nbz)
    f32 = jnp.float32

    def per_device(*args):
        dma = pltpu.SemaphoreType.DMA
        extended = pltpu.VMEM((22, ROWS, CZ), f32)
        values = pltpu.VMEM((6, 22, ROWS, CZ), f32)
        shifted = pltpu.VMEM((6, 22, ROWS + 16, CZ), f32)
        out = pl.pallas_call(
            functools.partial(kernel, (nbx, nby, nbz)),
            out_shape=jax.ShapeDtypeStruct((5, CX, CY, CZ), f32),
            in_specs=[pl.BlockSpec(memory_space=pltpu.HBM)] * 4,
            out_specs=pl.BlockSpec(memory_space=pltpu.VMEM),
            scratch_shapes=[
                values,
                extended, extended, extended, extended, extended, extended,
                pltpu.VMEM((22, ROWS, CZ), jnp.int32),
                pltpu.VMEM((22, ROWS, CZ), jnp.int32),
                pltpu.VMEM((CX, CY, CZ), jnp.int32),
                pltpu.VMEM((CX, CY, CZ), jnp.int32),
                pltpu.VMEM((2, CX, 8, CZ), f32),
                pltpu.VMEM((2, 20, 8, CZ), f32),
                pltpu.VMEM((4, ROWS, CZ), f32),
                pltpu.VMEM((2, 4, ROWS, CZ), f32),
                pltpu.VMEM((CY, CZ), f32),
                pltpu.VMEM((2, ROWS, CZ), f32),
                pltpu.VMEM((2, 2, ROWS, CZ), f32),
                pltpu.VMEM((6, ROWS, CZ), f32),
                shifted, shifted, shifted,
                extended,
                values,
                dma((4,)), dma((2, 2)), dma((2, 2)), dma((2, 2)), dma((2, 2)), dma((2,)), dma((2,)), dma((2,)), dma((2,)),
                dma((2, 2)), dma((2, 2)), dma((2,)), dma((2,)), dma((2,)), dma((2,)), dma((2, 3)), dma((2, 3)),
            ],
            compiler_params=pltpu.CompilerParams(
                collective_id=0, has_side_effects=True, vmem_limit_bytes=30 * 1024 * 1024
            ),
        )(*(pltpu.with_memory_space_constraint(a[0], pltpu.HBM) for a in args))
        return out[None]

    return jax.shard_map(
        per_device,
        mesh=mesh,
        in_specs=(
            P("boxes", None, None, None, None),
            P("boxes", None, None, None),
            P("boxes", None, None, None),
            P("boxes", None, None, None),
        ),
        out_specs=P("boxes", None, None, None, None),
        check_vma=False,
    )
```

```python
import functools

import jax
import jax.numpy as jnp
from jax import lax
from jax.experimental import pallas as pl
from jax.experimental.pallas import tpu as pltpu
from jax.sharding import PartitionSpec as P

NBY = 4
NBZ = 4
CX, CY, CZ = 16, 32, 128
MESH = pl.DeviceIdType.MESH

ROWS = 48
SLAB = 64
SLOT = 40
SIGNS = [(dx, dy) for dx in (-1, 0, 1) for dy in (-1, 0, 1)]


def lanes_of(shape):
    return lax.broadcasted_iota(jnp.int32, shape, len(shape) - 1)


def roll_lanes(a, by):
    return pltpu.roll(a, by % CZ, a.ndim - 1) if by % CZ else a


def roll_rows(a, by):
    return pltpu.roll(a, by % a.shape[0], 0) if by % a.shape[0] else a


def decode(code):
    xy = jnp.floor((code + 0.5) * (1.0 / 3.0))
    x = jnp.floor((code + 0.5) * (1.0 / 9.0))
    return xy, xy - 3.0 * x, code - 3.0 * xy


def towards(xy, y, dx, dy):
    if dy == 0:
        return xy >= 6.0 if dx == 1 else xy <= 2.0
    if dx == 0:
        return y == 1.0 + dy
    return xy == 3.0 * (dx + 1) + (dy + 1)


def moved(a, dx, dy):
    return roll_rows(roll_lanes(a, 2 * dx), dy)


def plane_spread(a, xy, y):
    up = towards(xy, y, 1, 0)
    down = towards(xy, y, -1, 0)

    def along_x(b):
        return b + moved(jnp.where(up, b, 0.0), 1, 0) + moved(jnp.where(down, b, 0.0), -1, 0)

    total = along_x(a)
    for dy in (-1, 1):
        total = total + moved(along_x(jnp.where(towards(xy, y, 0, dy), a, 0.0)), 0, dy)
    return total


def plane_gather(a, xy, y):
    left, right = towards(xy, y, 0, -1), towards(xy, y, 0, 1)

    def along_y(b):
        return b + jnp.where(right, moved(b, 0, -1), jnp.where(left, moved(b, 0, 1), 0.0))

    ahead, behind = along_y(moved(a, -1, 0)), along_y(moved(a, 1, 0))
    chosen = jnp.where(towards(xy, y, 1, 0), ahead, jnp.where(towards(xy, y, -1, 0), behind, 0.0))
    return along_y(a) + chosen


def in_all_slots(a, lane):
    return jnp.where(lane < SLOT, a, jnp.where(lane < 2 * SLOT, roll_lanes(a, SLOT), roll_lanes(a, 2 * SLOT)))


def rim_planes(own, ghost, lane):
    lower = lane % 2 == 1

    def signs(code):
        xy, y, z = decode(code)
        return xy, y, jnp.where(lower, z, 2.0 - z)

    near_own, far_own = signs(own[2]), signs(roll_lanes(own[2], -SLOT))
    near_ghost, far_ghost = signs(ghost[2]), signs(roll_lanes(ghost[2], -SLOT))
    one = jnp.ones(own[0].shape, jnp.float32)

    def spread_ones(plane, sign):
        xy, y, z = plane
        return plane_spread(one if sign == 0 else jnp.where(z == 1.0 + sign, 1.0, 0.0), xy, y)

    entering = spread_ones(near_ghost, 1)
    ghost_count = spread_ones(near_ghost, 0) + spread_ones(far_ghost, 1) + spread_ones(near_own, -1)
    own_count = spread_ones(near_own, 0) + entering + spread_ones(far_own, -1)
    last = lane >= 2 * SLOT

    def weighted(pack, count):
        w = in_all_slots(roll_lanes(pack[1], -2 * SLOT) / count, lane)
        return w * pack[0], w * jnp.where(last, 1.0, pack[1])

    ghost_w = weighted(ghost, ghost_count)
    own_w = weighted(own, own_count)
    xy, y, z = signs(in_all_slots(ghost[2], lane))
    sums = [plane_gather(a + b, xy, y) for a, b in zip(ghost_w, own_w)]
    volume = in_all_slots(roll_lanes(sums[1], -2 * SLOT), lane)
    deposits = [plane_spread(jnp.where(z == 2.0, s / volume, 0.0), xy, y) for s in sums]
    return entering, ghost_w, deposits


TILES = 5


def kernel(
    sizes, u_hbm, vf_hbm, mask_hbm, code_hbm, out_ref,
    uv, code, xy_v, y_v, z_v, xz_v, yz_v, ones_v, total_v, mask_raw, code_raw, y_send, y_recv, rim_own, rim_ghost, edge_send,
    edge_own, edge_ghost, rim_calc, w_v, up_v, down_v, inv_v, avg_v,
    load_sem, x_send_sem, x_recv_sem, y_send_sem, y_recv_sem, d_send_sem, d_recv_sem, z_send_sem, z_recv_sem,
    yz_send_sem, yz_recv_sem, ex_send_sem, ex_recv_sem, ey_send_sem, ey_recv_sem, ez_send_sem, ez_recv_sem,
):
    nbx, nby, nbz = sizes
    me = lax.axis_index("boxes")
    bx, by, bz = me // (nby * nbz), (me // nbz) % nby, me % nbz
    has_x = (bx > 0, bx < nbx - 1)
    has_y = (by > 0, by < nby - 1)
    has_z = (bz > 0, bz < nbz - 1)
    has_yz = [[has_y[j] & has_z[i] for i in (0, 1)] for j in (0, 1)]
    steps = (-1, 1)
    x_step, y_step = nby * nbz, nbz

    def when(cond):
        return pl.when(cond)

    barrier = pltpu.get_barrier_semaphore()
    greeted = 0
    for i in (0, 1):
        met = [(has_x[i], steps[i] * x_step), (has_y[i], steps[i] * y_step), (has_z[i], steps[i])]
        met += [(has_yz[j][i], steps[j] * y_step + steps[i]) for j in (0, 1)]
        for cond, step in met:
            @when(cond)
            def _(step=step):
                pl.semaphore_signal(barrier, inc=1, device_id=(me + step,), device_id_type=MESH)
            greeted = greeted + cond.astype(jnp.int32)

    loads = [
        pltpu.make_async_copy(mask_hbm, mask_raw, load_sem.at[0]),
        pltpu.make_async_copy(code_hbm, code_raw, load_sem.at[1]),
        pltpu.make_async_copy(vf_hbm, uv.at[0, 2:18, 8:40], load_sem.at[2]),
        pltpu.make_async_copy(u_hbm, uv.at[1:6, 2:18, 8:40], load_sem.at[3]),
    ]
    for load in loads:
        load.start()

    def remote(src, dst, send, recv, step):
        return pltpu.make_async_remote_copy(
            src_ref=src, dst_ref=dst, send_sem=send, recv_sem=recv, device_id=(me + step,), device_id_type=MESH)

    def x_copies(i):
        src_u, dst_u = (2, 18) if i == 0 else (17, 1)
        src_c, dst_c = (2, 18) if i == 0 else (16, 0)
        return [
            remote(uv.at[:, src_u, 8:40], uv.at[:, dst_u, 8:40], x_send_sem.at[i, 0], x_recv_sem.at[1 - i, 0],
                   steps[i] * x_step),
            remote(code.at[pl.ds(src_c, 2), 8:40], code.at[pl.ds(dst_c, 2), 8:40], x_send_sem.at[i, 1],
                   x_recv_sem.at[1 - i, 1], steps[i] * x_step),
        ]

    def d_copy(i):
        src, dst = (2, 18) if i == 0 else (16, 0)
        return remote(y_recv.at[:, pl.ds(src, 2)], y_recv.at[:, pl.ds(dst, 2)], d_send_sem.at[i], d_recv_sem.at[1 - i],
                      steps[i] * x_step)

    rim_src, rim_dst = (8, 32), (40, 0)

    def y_copies(i, which=None):
        return [
            remote(y_send.at[i], y_recv.at[1 - i, 2:18], y_send_sem.at[i, 0], y_recv_sem.at[1 - i, 0], steps[i] * y_step),
        ] * (which != 1) + [
            remote(rim_own.at[0:3, pl.ds(rim_src[i], 8)], rim_own.at[0:3, pl.ds(rim_dst[i], 8)], y_send_sem.at[i, 1],
                   y_recv_sem.at[1 - i, 1], steps[i] * y_step),
        ] * (which != 0)

    def z_copy(i):
        return remote(rim_own.at[0:3, 8:40], rim_ghost.at[1 - i, 0:3, 8:40], z_send_sem.at[i], z_recv_sem.at[1 - i], steps[i])

    def yz_copy(j, i):
        return remote(
            rim_own.at[0:3, pl.ds(rim_src[j], 8)], rim_ghost.at[1 - i, 0:3, pl.ds(rim_dst[j], 8)], yz_send_sem.at[j, i],
            yz_recv_sem.at[1 - j, 1 - i], steps[j] * y_step + steps[i])

    def ex_copy(i):
        return remote(edge_send, edge_own.at[1 - i, 8:40], ex_send_sem.at[i], ex_recv_sem.at[1 - i], steps[i] * x_step)

    def ey_copy(i):
        return remote(edge_own.at[:, pl.ds(rim_src[i], 8)], edge_own.at[:, pl.ds(rim_dst[i], 8)], ey_send_sem.at[i],
                      ey_recv_sem.at[1 - i], steps[i] * y_step)

    def ez_copy(i, part):
        rows = pl.ds((8, 0, 40)[part], (32, 8, 8)[part])
        return remote(edge_own.at[:, rows], edge_ghost.at[1 - i, :, rows], ez_send_sem.at[i, part],
                      ez_recv_sem.at[1 - i, part], steps[i])

    loads[0].wait()
    loads[1].wait()

    def write_signs(X, base):
        rows = pl.ds(base, 8)
        c = code[X, rows, :]
        xy, y, z = decode(c)
        xy_v[X, rows, :] = xy
        y_v[X, rows, :] = y
        z_v[X, rows, :] = z
        xz_v[X, rows, :] = xy - y + z
        yz_v[X, rows, :] = 3.0 * y + z
        ones_v[X, rows, :] = jnp.where(z == 2.0, 257, jnp.where(z == 0.0, 65537, 1))

    def own_codes(x, _):
        code[x + 2, 8:40, :] = jnp.where(mask_raw[x] == 1, code_raw[x], 13).astype(jnp.float32)
        return _

    lax.fori_loop(0, CX, own_codes, 0)
    loads[2].wait()
    loads[3].wait()

    def pack_y(x, _):
        for s, near, far in ((0, 8, 9), (1, 39, 38)):
            for q in range(6):
                y_send[s, x, q:q + 1, :] = uv[q, x + 2, near:near + 1, :]
            y_send[s, x, 6:7, :] = code[x + 2, near:near + 1, :]
            y_send[s, x, 7:8, :] = code[x + 2, far:far + 1, :]
        return _

    lax.fori_loop(0, CX, pack_y, 0)
    lane8 = lanes_of((8, CZ))

    def pack_rims(rim, slabs, base):
        blocks = [jnp.zeros((8, CZ), jnp.float32) for _ in range(3)]

        def place(b, value, slot, X):
            lane = slot * SLOT + 2 * X
            blocks[b] = jnp.where(lane8 // 2 == lane // 2, roll_lanes(value, lane + 1), blocks[b])

        for X in slabs:
            near = code[X, pl.ds(base, 8), :]
            place(2, near, 0, X)
            place(2, jnp.where(lane8 == CZ - 1, roll_lanes(near, 1), roll_lanes(near, -1)), 1, X)
            if 1 <= X <= 18:
                for q in range(5):
                    place(q // 3, uv[q + 1, X, pl.ds(base, 8), :], q % 3, X)
                place(1, uv[0, X, pl.ds(base, 8), :], 2, X)
        for b in range(3):
            rim[b, pl.ds(base, 8), :] = blocks[b]

    def pack_own_rims(t, _):
        pack_rims(rim_own, range(2, 18), pl.multiple_of(8 + 8 * t, 8))
        return _

    lax.fori_loop(0, 4, pack_own_rims, 0)

    lane32 = lanes_of((CY, CZ))
    kept = ((lane32 % SLOT) // 4 == 1) | ((lane32 % SLOT) // 4 == 8)
    compact = jnp.zeros((CY, CZ), jnp.float32)
    for b in range(3):
        compact = compact + roll_lanes(jnp.where(kept & (lane32 < (2 if b == 2 else 3) * SLOT), rim_own[b, 8:40, :], 0.0), 8 * b)
    edge_send[...] = compact
    pl.semaphore_wait(barrier, greeted)

    for i in (0, 1):
        @when(has_z[i])
        def _(i=i):
            z_copy(i).start()
    for i in (0, 1):
        @when(has_x[i])
        def _(i=i):
            ex_copy(i).start()
    for i in (0, 1):
        @when(has_y[i])
        def _(i=i):
            for copy in y_copies(i):
                copy.start()

        for j in (0, 1):
            @when(has_yz[j][i])
            def _(i=i, j=j):
                yz_copy(j, i).start()
    for i in (0, 1):
        @when(has_x[i])
        def _(i=i):
            for copy in x_copies(i):
                copy.start()

    tile_row = lax.broadcasted_iota(jnp.int32, (8, CZ), 0)

    def blank_rim(rim, first, rows):
        for b in range(3):
            rim[b, first:first + rows, :] = jnp.full((rows, CZ), 13.0 if b == 2 else 0.0, jnp.float32)

    def blank_edge(rows):
        spot = lanes_of((rows, CZ)) - 16
        is_code = (spot >= 0) & (spot < 2 * SLOT) & (((spot % SLOT) // 4 == 1) | ((spot % SLOT) // 4 == 8))
        return jnp.where(is_code, 13.0, 0.0)

    for s in (0, 1):
        @when(jnp.logical_not(has_y[s]))
        def _(s=s):
            for side in (0, 1):
                edge_own[side, 40 * s:40 * s + 8, :] = blank_edge(8)
            blank_rim(rim_own, 0 if s == 0 else 40, 8)
            for X in range(2, 18):
                y_recv[s, X] = jnp.where(tile_row < 6, 0.0, 13.0)

        @when(jnp.logical_not(has_z[s]))
        def _(s=s):
            blank_rim(rim_ghost.at[s], 8, 32)
            for side in (0, 1):
                edge_ghost[s, side] = blank_edge(ROWS)

        for j in (0, 1):
            @when(jnp.logical_not(has_yz[j][s]))
            def _(s=s, j=j):
                blank_rim(rim_ghost.at[s], 0 if j == 0 else 40, 8)

        @when(jnp.logical_not(has_x[s]))
        def _(s=s):
            u_at, c_at = (1, 0) if s == 0 else (18, 18)
            edge_own[s, 8:40, :] = blank_edge(CY)
            for q in range(6):
                uv[q, u_at, 8:40, :] = jnp.zeros((CY, CZ), jnp.float32)
            for c in (0, 1):
                code[c_at + c, 8:40, :] = jnp.full((CY, CZ), 13.0, jnp.float32)
                for j in (0, 1):
                    y_recv[j, c_at + c] = jnp.where(tile_row < 6, 0.0, 13.0)

    def count(X, tiles):
        for t in tiles:
            top = 7 + 8 * t
            total = ones_v[X, top:top + 8, :]
            for dx, dy in SIGNS:
                if (dx, dy) != (0, 0):
                    at = slice(top - dy, top - dy + 8)
                    signs = (y_v if dx == 0 else xy_v)[X - dx, at, :]
                    total = total + jnp.where(towards(signs, signs, dx, dy), ones_v[X - dx, at, :], 0)
            total_v[X, top:top + 8, :] = total

    first, final = lane8 == 0, lane8 == CZ - 1

    def at_edges(k, slot, X, top):
        shift = CZ * 2 - (slot * SLOT + 2 * X + 1)
        return pltpu.roll(rim_calc[k, pl.ds(top, 8), :], lax.rem(shift, CZ), 1)

    def weigh(X, tiles=range(TILES)):
        for t in tiles:
            top = 7 + 8 * t
            rows = pl.ds(top, 8)
            total = total_v[X, rows, :]
            here = (total & 255).astype(jnp.float32)
            up = ((total >> 8) & 255).astype(jnp.float32)
            down = (total >> 16).astype(jnp.float32)
            edge = at_edges(0, 0, X, top)
            inv = 1.0 / (here + jnp.where(first, edge, roll_lanes(up, 1)) + jnp.where(final, edge, roll_lanes(down, -1)))
            inv_v[X, rows, :] = inv
            w = uv[0, X, rows, :] * inv
            for q in range(6):
                value = w if q == 0 else w * uv[q, X, rows, :]
                k, slot = (2, 2) if q == 0 else (1 + (q - 1) // 3, (q - 1) % 3)
                edge = at_edges(k, slot, X, top)
                w_v[q, X, rows, :] = value
                up_v[q, X, pl.ds(top + 8, 8), :] = value + jnp.where(final, edge, roll_lanes(value, -1))
                down_v[q, X, pl.ds(top + 16, 8), :] = value + jnp.where(first, edge, roll_lanes(value, 1))

    def gather(start, slabs, t):
        top = 7 + 8 * t
        rows = pl.ds(top, 8)

        def step(X, behind, here, ahead):
            targets = []
            for dx, use in ((1, behind), (0, here), (-1, ahead)):
                if use is not None:
                    y, z = y_v[X - dx, rows, :], z_v[X - dx, rows, :]
                    along = None if dx == 0 else towards(xy_v[X - dx, rows, :], None, dx, 0)
                    targets.append((dx, along, y == 2.0, y == 0.0, z == 2.0, z == 0.0))
            new = {dx: [] for dx, *_ in targets}
            for q in range(6):
                lines = [[ref[q, X, pl.ds(top + dy + shift, 8), :] for ref, shift in ((up_v, 8), (down_v, 16), (w_v, 0))] for dy in (-1, 0, 1)]
                for dx, along, y_up, y_down, z_up, z_down in targets:
                    low, mid, high = (jnp.where(z_up, a, jnp.where(z_down, b, c)) for a, b, c in lines)
                    plane = mid + jnp.where(y_up, high, jnp.where(y_down, low, 0.0))
                    if along is not None:
                        plane = jnp.where(along, plane, 0.0)
                    old = {1: behind, 0: here, -1: ahead}[dx][q]
                    new[dx].append(plane if old is None else old + plane)
            return new

        none = [None] * 6
        one = step(start - 1, None, None, none)[-1]
        both = step(start, None, one, none)

        def walk(X, sums):
            new = step(X, list(sums[:6]), list(sums[6:]), none)
            inv = 1.0 / new[1][0]
            for q in range(5):
                avg_v[q, X - 1, pl.ds(top + 8 * (q % 3), 8), :] = new[1][q + 1] * inv
            return (*new[0], *new[-1])

        lax.fori_loop(start + 1, start + slabs + 1, walk, (*both[0], *both[-1]))

    def scatter(X, tiles=range(4)):
        for t in tiles:
            top = 8 + 8 * t
            here, up, down = [None] * 5, [None] * 5, [None] * 5
            for dx, dy in SIGNS:
                at = pl.ds(top - dy, 8)
                if (dx, dy) == (0, 0):
                    z = z_v[X, at, :]
                    hit, z_up, z_down = None, z == 2.0, z == 0.0
                else:
                    signs = (y_v if dx == 0 else xy_v)[X - dx, at, :]
                    hit = towards(signs, signs, dx, dy)
                    z = (code if dx * dy else yz_v if dx == 0 else xz_v)[X - dx, at, :]
                    full = 9 * (dx + 1) + 3 * (dy + 1) if dx * dy else 3 * (dx + dy + 1)
                    z_up, z_down = z == full + 2.0, z == full + 0.0
                for q in range(5):
                    a = avg_v[q, X - dx, pl.ds(top - dy + 8 * (q % 3), 8), :]
                    terms = (a if hit is None else jnp.where(hit, a, 0.0), jnp.where(z_up, a, 0.0), jnp.where(z_down, a, 0.0))
                    here[q], up[q], down[q] = (
                        new if old is None else old + new for old, new in zip((here[q], up[q], down[q]), terms))
            inv = inv_v[X, pl.ds(top, 8), :]
            for q in range(5):
                edge = at_edges(3 + q // 3, q % 3, X, top)
                total = here[q] + jnp.where(first, edge, roll_lanes(up[q], 1)) + jnp.where(
                    final, edge, roll_lanes(down[q], -1))
                out_ref[q, X - 2, pl.ds(8 * t if isinstance(t, int) else pl.multiple_of(8 * t, 8), 8), :] = total * inv

    def loop(lo, hi, body):
        def step(k, _):
            body(k)
            return _

        lax.fori_loop(lo, hi, step, 0)

    def both_ends(k, low, high):
        return k + low + (k // 2) * (high - low - 2)

    def unpack_y(X, fields):
        for s, near, far in ((0, 7, 6), (1, 40, 41)):
            code[X, near:near + 1, :] = y_recv[s, X, 6:7, :]
            code[X, far:far + 1, :] = y_recv[s, X, 7:8, :]
            if fields:
                for q in range(6):
                    uv[q, X, near:near + 1, :] = y_recv[s, X, q:q + 1, :]

    near_rows = slice(4, 44)
    lane = lanes_of((40, CZ))

    def planes(own, from_lower, from_upper, inner=False):
        lane = lanes_of(own[0].shape)
        ghost = [jnp.where(lane % 2 == 1, roll_lanes(a, 1), roll_lanes(b, -1)) for a, b in zip(from_lower, from_upper)]
        entering, ghost_w, deposits = rim_planes(own, ghost, lane)
        for k, a in enumerate((entering, *ghost_w) if inner else (entering, *ghost_w, *deposits)):
            rim_calc[k, slice(8, 40) if inner else near_rows, :] = a

    def own_signs(X):
        for t in range(4):
            write_signs(X, 8 + 8 * t)

    loop(2, 18, own_signs)
    loop(3, 17, lambda X: count(X, (1, 2, 3)))

    for s in (0, 1):
        @when(has_z[s])
        def _(s=s):
            z_copy(1 - s).wait_recv()
    planes(*([rim[b, 8:40, :] for b in range(3)] for rim in (rim_own, rim_ghost.at[0], rim_ghost.at[1])), inner=True)
    loop(0, 7, lambda k: [weigh(3 + 2 * k + i, (1, 2, 3)) for i in (0, 1)])
    gather(4, 12, 2)

    for s in (0, 1):
        @when(has_y[s])
        def _(s=s):
            y_copies(1 - s, 0)[0].wait_recv()
    for i in (0, 1):
        @when(has_x[i])
        def _(i=i):
            d_copy(i).start()

    def y_ghosts(X):
        unpack_y(X, True)

    loop(2, 18, y_ghosts)

    def ghost_signs(X):
        write_signs(X, 0)
        write_signs(X, 40)

    loop(2, 18, ghost_signs)
    loop(3, 17, lambda X: count(X, (0, 4)))

    for s in (0, 1):
        @when(has_x[s])
        def _(s=s):
            ex_copy(1 - s).wait_recv()
    for i in (0, 1):
        @when(has_y[i])
        def _(i=i):
            ey_copy(i).start()

        @when(has_z[i])
        def _(i=i):
            ez_copy(i, 0).start()

    for s in (0, 1):
        @when(has_y[s])
        def _(s=s):
            y_copies(1 - s, 1)[0].wait_recv()

        for j in (0, 1):
            @when(has_yz[j][s])
            def _(s=s, j=j):
                yz_copy(1 - j, 1 - s).wait_recv()
    planes(*([rim[b, near_rows, :] for b in range(3)] for rim in (rim_own, rim_ghost.at[0], rim_ghost.at[1])))

    loop(0, 7, lambda k: [weigh(3 + 2 * k + i, (0, 4)) for i in (0, 1)])
    for s in (0, 1):
        @when(has_y[s])
        def _(s=s):
            ey_copy(1 - s).wait_recv()
    for i in (0, 1):
        @when(has_z[i])
        def _(i=i):
            ez_copy(i, 1).start()
            ez_copy(i, 2).start()
    loop(0, TILES - 1, lambda k: gather(4, 12, k + k // 2))
    loop(5, 15, scatter)

    for s in (0, 1):
        @when(has_z[s])
        def _(s=s):
            for part in range(3):
                ez_copy(1 - s, part).wait_recv()
    place = lane % SLOT
    at_x = (place < 4) | (place >= 36)

    def with_x(rim, edge):
        low, high = edge[0, near_rows, :], edge[1, near_rows, :]
        return [
            jnp.where(at_x, jnp.where(place < 4, roll_lanes(low, -(32 + 8 * b)), roll_lanes(high, 32 - 8 * b)), rim[b, near_rows, :])
            for b in range(3)
        ]

    planes(with_x(rim_own, edge_own), *(with_x(rim_ghost.at[s], edge_ghost.at[s]) for s in (0, 1)))

    for s in (0, 1):
        @when(has_x[s])
        def _(s=s):
            for copy in x_copies(1 - s):
                copy.wait_recv()
            d_copy(1 - s).wait_recv()

    loop(0, 2, lambda k: unpack_y(1 + 17 * k, True))
    loop(0, 2, lambda k: unpack_y(19 * k, False))

    def end_signs(k):
        for t in range(6):
            write_signs(both_ends(k, 0, 18), 8 * t)

    loop(0, 4, end_signs)
    loop(0, 4, lambda k: count(both_ends(k, 1, 17), range(TILES)))
    loop(0, 4, lambda k: weigh(both_ends(k, 1, 17)))
    loop(0, 2 * TILES, lambda k: gather(1 + 15 * (k // TILES), 3, k % TILES))
    loop(0, 6, lambda k: scatter(2 + k + 10 * (k // 3)))

    for i in (0, 1):
        @when(has_x[i])
        def _(i=i):
            for copy in (*x_copies(i), d_copy(i), ex_copy(i)):
                copy.wait_send()

        @when(has_y[i])
        def _(i=i):
            for copy in (*y_copies(i), ey_copy(i)):
                copy.wait_send()

        @when(has_z[i])
        def _(i=i):
            for copy in (z_copy(i), *(ez_copy(i, part) for part in range(3))):
                copy.wait_send()

        for j in (0, 1):
            @when(has_yz[j][i])
            def _(i=i, j=j):
                yz_copy(j, i).wait_send()


def solution(mesh, nby=NBY, nbz=NBZ):
    nbx = mesh.shape["boxes"] // (nby * nbz)
    f32 = jnp.float32

    def per_device(*args):
        dma = pltpu.SemaphoreType.DMA
        extended = pltpu.VMEM((22, SLAB, CZ), f32)
        values = pltpu.VMEM((6, 22, SLAB, CZ), f32)
        out = pl.pallas_call(
            functools.partial(kernel, (nbx, nby, nbz)),
            out_shape=jax.ShapeDtypeStruct((5, CX, CY, CZ), f32),
            in_specs=[pl.BlockSpec(memory_space=pltpu.HBM)] * 4,
            out_specs=pl.BlockSpec(memory_space=pltpu.VMEM),
            scratch_shapes=[
                values,
                extended, extended, extended, extended, extended, extended,
                pltpu.VMEM((22, SLAB, CZ), jnp.int32),
                pltpu.VMEM((22, SLAB, CZ), jnp.int32),
                pltpu.VMEM((CX, CY, CZ), jnp.int32),
                pltpu.VMEM((CX, CY, CZ), jnp.int32),
                pltpu.VMEM((2, CX, 8, CZ), f32),
                pltpu.VMEM((2, 20, 8, CZ), f32),
                pltpu.VMEM((4, ROWS, CZ), f32),
                pltpu.VMEM((2, 4, ROWS, CZ), f32),
                pltpu.VMEM((CY, CZ), f32),
                pltpu.VMEM((2, ROWS, CZ), f32),
                pltpu.VMEM((2, 2, ROWS, CZ), f32),
                pltpu.VMEM((6, ROWS, CZ), f32),
                values, values, values,
                extended,
                values,
                dma((4,)), dma((2, 2)), dma((2, 2)), dma((2, 2)), dma((2, 2)), dma((2,)), dma((2,)), dma((2,)), dma((2,)),
                dma((2, 2)), dma((2, 2)), dma((2,)), dma((2,)), dma((2,)), dma((2,)), dma((2, 3)), dma((2, 3)),
            ],
            compiler_params=pltpu.CompilerParams(
                collective_id=0, has_side_effects=True, vmem_limit_bytes=38 * 1024 * 1024
            ),
        )(*(pltpu.with_memory_space_constraint(a[0], pltpu.HBM) for a in args))
        return out[None]

    return jax.shard_map(
        per_device,
        mesh=mesh,
        in_specs=(
            P("boxes", None, None, None, None),
            P("boxes", None, None, None),
            P("boxes", None, None, None),
            P("boxes", None, None, None),
        ),
        out_specs=P("boxes", None, None, None, None),
        check_vma=False,
    )
```

```python
import functools

import jax
import jax.numpy as jnp
from jax import lax
from jax.experimental import pallas as pl
from jax.experimental.pallas import tpu as pltpu
from jax.sharding import PartitionSpec as P

NBY = 4
NBZ = 4
CX, CY, CZ = 16, 32, 128
MESH = pl.DeviceIdType.MESH

ROWS = 48
SLAB = 64
SLOT = 40
SIGNS = [(dx, dy) for dx in (-1, 0, 1) for dy in (-1, 0, 1)]


def lanes_of(shape):
    return lax.broadcasted_iota(jnp.int32, shape, len(shape) - 1)


def roll_lanes(a, by):
    return pltpu.roll(a, by % CZ, a.ndim - 1) if by % CZ else a


def roll_rows(a, by):
    return pltpu.roll(a, by % a.shape[0], 0) if by % a.shape[0] else a


def decode(code):
    xy = jnp.floor((code + 0.5) * (1.0 / 3.0))
    x = jnp.floor((code + 0.5) * (1.0 / 9.0))
    return xy, xy - 3.0 * x, code - 3.0 * xy


def towards(xy, y, dx, dy):
    if dy == 0:
        return xy >= 6.0 if dx == 1 else xy <= 2.0
    if dx == 0:
        return y == 1.0 + dy
    return xy == 3.0 * (dx + 1) + (dy + 1)


def moved(a, dx, dy):
    return roll_rows(roll_lanes(a, 2 * dx), dy)


def plane_spread(a, xy, y):
    up = towards(xy, y, 1, 0)
    down = towards(xy, y, -1, 0)

    def along_x(b):
        return b + moved(jnp.where(up, b, 0.0), 1, 0) + moved(jnp.where(down, b, 0.0), -1, 0)

    total = along_x(a)
    for dy in (-1, 1):
        total = total + moved(along_x(jnp.where(towards(xy, y, 0, dy), a, 0.0)), 0, dy)
    return total


def plane_gather(a, xy, y):
    left, right = towards(xy, y, 0, -1), towards(xy, y, 0, 1)

    def along_y(b):
        return b + jnp.where(right, moved(b, 0, -1), jnp.where(left, moved(b, 0, 1), 0.0))

    ahead, behind = along_y(moved(a, -1, 0)), along_y(moved(a, 1, 0))
    chosen = jnp.where(towards(xy, y, 1, 0), ahead, jnp.where(towards(xy, y, -1, 0), behind, 0.0))
    return along_y(a) + chosen


def in_all_slots(a, lane):
    return jnp.where(lane < SLOT, a, jnp.where(lane < 2 * SLOT, roll_lanes(a, SLOT), roll_lanes(a, 2 * SLOT)))


def rim_planes(own, ghost, lane):
    lower = lane % 2 == 1

    def signs(code):
        xy, y, z = decode(code)
        return xy, y, jnp.where(lower, z, 2.0 - z)

    near_own, far_own = signs(own[2]), signs(roll_lanes(own[2], -SLOT))
    near_ghost, far_ghost = signs(ghost[2]), signs(roll_lanes(ghost[2], -SLOT))
    one = jnp.ones(own[0].shape, jnp.float32)

    def spread_ones(plane, sign):
        xy, y, z = plane
        return plane_spread(one if sign == 0 else jnp.where(z == 1.0 + sign, 1.0, 0.0), xy, y)

    entering = spread_ones(near_ghost, 1)
    ghost_count = spread_ones(near_ghost, 0) + spread_ones(far_ghost, 1) + spread_ones(near_own, -1)
    own_count = spread_ones(near_own, 0) + entering + spread_ones(far_own, -1)
    last = lane >= 2 * SLOT

    def weighted(pack, count):
        w = in_all_slots(roll_lanes(pack[1], -2 * SLOT) / count, lane)
        return w * pack[0], w * jnp.where(last, 1.0, pack[1])

    ghost_w = weighted(ghost, ghost_count)
    own_w = weighted(own, own_count)
    xy, y, z = signs(in_all_slots(ghost[2], lane))
    sums = [plane_gather(a + b, xy, y) for a, b in zip(ghost_w, own_w)]
    volume = in_all_slots(roll_lanes(sums[1], -2 * SLOT), lane)
    deposits = [plane_spread(jnp.where(z == 2.0, s / volume, 0.0), xy, y) for s in sums]
    return entering, ghost_w, deposits


TILES = 5


def kernel(
    sizes, u_hbm, vf_hbm, mask_hbm, code_hbm, out_ref,
    uv, code, xy_v, y_v, z_v, xz_v, yz_v, ones_v, total_v, mask_raw, code_raw, y_send, y_recv, rim_own, rim_ghost, edge_send,
    edge_own, edge_ghost, rim_calc, w_v, up_v, down_v, inv_v, avg_v,
    load_sem, x_send_sem, x_recv_sem, y_send_sem, y_recv_sem, d_send_sem, d_recv_sem, z_send_sem, z_recv_sem,
    yz_send_sem, yz_recv_sem, ex_send_sem, ex_recv_sem, ey_send_sem, ey_recv_sem, ez_send_sem, ez_recv_sem,
):
    nbx, nby, nbz = sizes
    me = lax.axis_index("boxes")
    bx, by, bz = me // (nby * nbz), (me // nbz) % nby, me % nbz
    has_x = (bx > 0, bx < nbx - 1)
    has_y = (by > 0, by < nby - 1)
    has_z = (bz > 0, bz < nbz - 1)
    has_yz = [[has_y[j] & has_z[i] for i in (0, 1)] for j in (0, 1)]
    steps = (-1, 1)
    x_step, y_step = nby * nbz, nbz

    def when(cond):
        return pl.when(cond)

    barrier = pltpu.get_barrier_semaphore()
    greeted = 0
    for i in (0, 1):
        met = [(has_x[i], steps[i] * x_step), (has_y[i], steps[i] * y_step), (has_z[i], steps[i])]
        met += [(has_yz[j][i], steps[j] * y_step + steps[i]) for j in (0, 1)]
        for cond, step in met:
            @when(cond)
            def _(step=step):
                pl.semaphore_signal(barrier, inc=1, device_id=(me + step,), device_id_type=MESH)
            greeted = greeted + cond.astype(jnp.int32)

    loads = [
        pltpu.make_async_copy(mask_hbm, mask_raw, load_sem.at[0]),
        pltpu.make_async_copy(code_hbm, code_raw, load_sem.at[1]),
        pltpu.make_async_copy(vf_hbm, uv.at[0, 2:18, 8:40], load_sem.at[2]),
        pltpu.make_async_copy(u_hbm, uv.at[1:6, 2:18, 8:40], load_sem.at[3]),
    ]
    for load in loads:
        load.start()

    def remote(src, dst, send, recv, step):
        return pltpu.make_async_remote_copy(
            src_ref=src, dst_ref=dst, send_sem=send, recv_sem=recv, device_id=(me + step,), device_id_type=MESH)

    def x_copies(i):
        src_u, dst_u = (2, 18) if i == 0 else (17, 1)
        src_c, dst_c = (2, 18) if i == 0 else (16, 0)
        return [
            remote(uv.at[:, src_u, 8:40], uv.at[:, dst_u, 8:40], x_send_sem.at[i, 0], x_recv_sem.at[1 - i, 0],
                   steps[i] * x_step),
            remote(code.at[pl.ds(src_c, 2), 8:40], code.at[pl.ds(dst_c, 2), 8:40], x_send_sem.at[i, 1],
                   x_recv_sem.at[1 - i, 1], steps[i] * x_step),
        ]

    def d_copy(i):
        src, dst = (2, 18) if i == 0 else (16, 0)
        return remote(y_recv.at[:, pl.ds(src, 2)], y_recv.at[:, pl.ds(dst, 2)], d_send_sem.at[i], d_recv_sem.at[1 - i],
                      steps[i] * x_step)

    rim_src, rim_dst = (8, 32), (40, 0)

    def y_copies(i, which=None):
        return [
            remote(y_send.at[i], y_recv.at[1 - i, 2:18], y_send_sem.at[i, 0], y_recv_sem.at[1 - i, 0], steps[i] * y_step),
        ] * (which != 1) + [
            remote(rim_own.at[0:3, pl.ds(rim_src[i], 8)], rim_own.at[0:3, pl.ds(rim_dst[i], 8)], y_send_sem.at[i, 1],
                   y_recv_sem.at[1 - i, 1], steps[i] * y_step),
        ] * (which != 0)

    def z_copy(i):
        return remote(rim_own.at[0:3, 8:40], rim_ghost.at[1 - i, 0:3, 8:40], z_send_sem.at[i], z_recv_sem.at[1 - i], steps[i])

    def yz_copy(j, i):
        return remote(
            rim_own.at[0:3, pl.ds(rim_src[j], 8)], rim_ghost.at[1 - i, 0:3, pl.ds(rim_dst[j], 8)], yz_send_sem.at[j, i],
            yz_recv_sem.at[1 - j, 1 - i], steps[j] * y_step + steps[i])

    def ex_copy(i):
        return remote(edge_send, edge_own.at[1 - i, 8:40], ex_send_sem.at[i], ex_recv_sem.at[1 - i], steps[i] * x_step)

    def ey_copy(i):
        return remote(edge_own.at[:, pl.ds(rim_src[i], 8)], edge_own.at[:, pl.ds(rim_dst[i], 8)], ey_send_sem.at[i],
                      ey_recv_sem.at[1 - i], steps[i] * y_step)

    def ez_copy(i, part):
        rows = pl.ds((8, 0, 40)[part], (32, 8, 8)[part])
        return remote(edge_own.at[:, rows], edge_ghost.at[1 - i, :, rows], ez_send_sem.at[i, part],
                      ez_recv_sem.at[1 - i, part], steps[i])

    loads[0].wait()
    loads[1].wait()

    def write_signs(X, base):
        rows = pl.ds(base, 8)
        c = code[X, rows, :]
        xy, y, z = decode(c)
        xy_v[X, rows, :] = xy
        y_v[X, rows, :] = y
        z_v[X, rows, :] = z
        xz_v[X, rows, :] = xy - y + z
        yz_v[X, rows, :] = 3.0 * y + z
        ones_v[X, rows, :] = jnp.where(z == 2.0, 257, jnp.where(z == 0.0, 65537, 1))

    def own_codes(x, _):
        code[x + 2, 8:40, :] = jnp.where(mask_raw[x] == 1, code_raw[x], 13).astype(jnp.float32)
        return _

    lax.fori_loop(0, CX, own_codes, 0)
    loads[2].wait()
    loads[3].wait()

    def pack_y(x, _):
        for s, near, far in ((0, 8, 9), (1, 39, 38)):
            for q in range(6):
                y_send[s, x, q:q + 1, :] = uv[q, x + 2, near:near + 1, :]
            y_send[s, x, 6:7, :] = code[x + 2, near:near + 1, :]
            y_send[s, x, 7:8, :] = code[x + 2, far:far + 1, :]
        return _

    lax.fori_loop(0, CX, pack_y, 0)
    lane8 = lanes_of((8, CZ))

    def pack_rims(rim, slabs, base):
        blocks = [jnp.zeros((8, CZ), jnp.float32) for _ in range(3)]

        def place(b, value, slot, X):
            lane = slot * SLOT + 2 * X
            blocks[b] = jnp.where(lane8 // 2 == lane // 2, roll_lanes(value, lane + 1), blocks[b])

        for X in slabs:
            near = code[X, pl.ds(base, 8), :]
            place(2, near, 0, X)
            place(2, jnp.where(lane8 == CZ - 1, roll_lanes(near, 1), roll_lanes(near, -1)), 1, X)
            if 1 <= X <= 18:
                for q in range(5):
                    place(q // 3, uv[q + 1, X, pl.ds(base, 8), :], q % 3, X)
                place(1, uv[0, X, pl.ds(base, 8), :], 2, X)
        for b in range(3):
            rim[b, pl.ds(base, 8), :] = blocks[b]

    def pack_own_rims(t, _):
        pack_rims(rim_own, range(2, 18), pl.multiple_of(8 + 8 * t, 8))
        return _

    lax.fori_loop(0, 4, pack_own_rims, 0)

    lane32 = lanes_of((CY, CZ))
    kept = ((lane32 % SLOT) // 4 == 1) | ((lane32 % SLOT) // 4 == 8)
    compact = jnp.zeros((CY, CZ), jnp.float32)
    for b in range(3):
        compact = compact + roll_lanes(jnp.where(kept & (lane32 < (2 if b == 2 else 3) * SLOT), rim_own[b, 8:40, :], 0.0), 8 * b)
    edge_send[...] = compact
    pl.semaphore_wait(barrier, greeted)

    for i in (0, 1):
        @when(has_z[i])
        def _(i=i):
            z_copy(i).start()
    for i in (0, 1):
        @when(has_x[i])
        def _(i=i):
            ex_copy(i).start()
    for i in (0, 1):
        @when(has_y[i])
        def _(i=i):
            for copy in y_copies(i):
                copy.start()

        for j in (0, 1):
            @when(has_yz[j][i])
            def _(i=i, j=j):
                yz_copy(j, i).start()
    for i in (0, 1):
        @when(has_x[i])
        def _(i=i):
            for copy in x_copies(i):
                copy.start()

    tile_row = lax.broadcasted_iota(jnp.int32, (8, CZ), 0)

    def blank_rim(rim, first, rows):
        for b in range(3):
            rim[b, first:first + rows, :] = jnp.full((rows, CZ), 13.0 if b == 2 else 0.0, jnp.float32)

    def blank_edge(rows):
        spot = lanes_of((rows, CZ)) - 16
        is_code = (spot >= 0) & (spot < 2 * SLOT) & (((spot % SLOT) // 4 == 1) | ((spot % SLOT) // 4 == 8))
        return jnp.where(is_code, 13.0, 0.0)

    for s in (0, 1):
        @when(jnp.logical_not(has_y[s]))
        def _(s=s):
            for side in (0, 1):
                edge_own[side, 40 * s:40 * s + 8, :] = blank_edge(8)
            blank_rim(rim_own, 0 if s == 0 else 40, 8)
            for X in range(2, 18):
                y_recv[s, X] = jnp.where(tile_row < 6, 0.0, 13.0)

        @when(jnp.logical_not(has_z[s]))
        def _(s=s):
            blank_rim(rim_ghost.at[s], 8, 32)
            for side in (0, 1):
                edge_ghost[s, side] = blank_edge(ROWS)

        for j in (0, 1):
            @when(jnp.logical_not(has_yz[j][s]))
            def _(s=s, j=j):
                blank_rim(rim_ghost.at[s], 0 if j == 0 else 40, 8)

        @when(jnp.logical_not(has_x[s]))
        def _(s=s):
            u_at, c_at = (1, 0) if s == 0 else (18, 18)
            edge_own[s, 8:40, :] = blank_edge(CY)
            for q in range(6):
                uv[q, u_at, 8:40, :] = jnp.zeros((CY, CZ), jnp.float32)
            for c in (0, 1):
                code[c_at + c, 8:40, :] = jnp.full((CY, CZ), 13.0, jnp.float32)
                for j in (0, 1):
                    y_recv[j, c_at + c] = jnp.where(tile_row < 6, 0.0, 13.0)

    def count(X, tiles):
        for t in tiles:
            top = 7 + 8 * t
            total = ones_v[X, top:top + 8, :]
            for dx, dy in SIGNS:
                if (dx, dy) != (0, 0):
                    at = slice(top - dy, top - dy + 8)
                    signs = (y_v if dx == 0 else xy_v)[X - dx, at, :]
                    total = total + jnp.where(towards(signs, signs, dx, dy), ones_v[X - dx, at, :], 0)
            total_v[X, top:top + 8, :] = total

    first, final = lane8 == 0, lane8 == CZ - 1

    def at_edges(k, slot, X, top):
        shift = CZ * 2 - (slot * SLOT + 2 * X + 1)
        return pltpu.roll(rim_calc[k, pl.ds(top, 8), :], lax.rem(shift, CZ), 1)

    def weigh(X, tiles=range(TILES)):
        for t in tiles:
            top = 7 + 8 * t
            rows = pl.ds(top, 8)
            total = total_v[X, rows, :]
            here = (total & 255).astype(jnp.float32)
            up = ((total >> 8) & 255).astype(jnp.float32)
            down = (total >> 16).astype(jnp.float32)
            edge = at_edges(0, 0, X, top)
            inv = 1.0 / (here + jnp.where(first, edge, roll_lanes(up, 1)) + jnp.where(final, edge, roll_lanes(down, -1)))
            inv_v[X, rows, :] = inv
            w = uv[0, X, rows, :] * inv
            for q in range(6):
                value = w if q == 0 else w * uv[q, X, rows, :]
                k, slot = (2, 2) if q == 0 else (1 + (q - 1) // 3, (q - 1) % 3)
                edge = at_edges(k, slot, X, top)
                w_v[q, X, rows, :] = value
                up_v[q, X, pl.ds(top + 8, 8), :] = value + jnp.where(final, edge, roll_lanes(value, -1))
                down_v[q, X, pl.ds(top + 16, 8), :] = value + jnp.where(first, edge, roll_lanes(value, 1))

    def gather(start, slabs, t):
        top = 7 + 8 * t
        rows = pl.ds(top, 8)

        def step(X, behind, here, ahead):
            targets = []
            for dx, use in ((1, behind), (0, here), (-1, ahead)):
                if use is not None:
                    y, z = y_v[X - dx, rows, :], z_v[X - dx, rows, :]
                    along = None if dx == 0 else towards(xy_v[X - dx, rows, :], None, dx, 0)
                    targets.append((dx, along, y == 2.0, y == 0.0, z == 2.0, z == 0.0))
            new = {dx: [] for dx, *_ in targets}
            for q in range(6):
                lines = [[ref[q, X, pl.ds(top + dy + shift, 8), :] for ref, shift in ((up_v, 8), (down_v, 16), (w_v, 0))] for dy in (-1, 0, 1)]
                for dx, along, y_up, y_down, z_up, z_down in targets:
                    low, mid, high = (jnp.where(z_up, a, jnp.where(z_down, b, c)) for a, b, c in lines)
                    plane = mid + jnp.where(y_up, high, jnp.where(y_down, low, 0.0))
                    if along is not None:
                        plane = jnp.where(along, plane, 0.0)
                    old = {1: behind, 0: here, -1: ahead}[dx][q]
                    new[dx].append(plane if old is None else old + plane)
            return new

        none = [None] * 6
        one = step(start - 1, None, None, none)[-1]
        both = step(start, None, one, none)

        def walk(X, sums):
            new = step(X, list(sums[:6]), list(sums[6:]), none)
            inv = 1.0 / new[1][0]
            for q in range(5):
                avg_v[q, X - 1, pl.ds(top + 8 * (q % 3), 8), :] = new[1][q + 1] * inv
            return (*new[0], *new[-1])

        def walk_on(k, sums):
            for i in range(3):
                sums = walk(start + 1 + 3 * k + i, sums)
            return sums

        lax.fori_loop(0, slabs // 3, walk_on, (*both[0], *both[-1]))

    def scatter(X, tiles=range(4)):
        for t in tiles:
            top = 8 + 8 * t
            here, up, down = [None] * 5, [None] * 5, [None] * 5
            for dx, dy in SIGNS:
                at = pl.ds(top - dy, 8)
                if (dx, dy) == (0, 0):
                    z = z_v[X, at, :]
                    hit, z_up, z_down = None, z == 2.0, z == 0.0
                else:
                    signs = (y_v if dx == 0 else xy_v)[X - dx, at, :]
                    hit = towards(signs, signs, dx, dy)
                    z = (code if dx * dy else yz_v if dx == 0 else xz_v)[X - dx, at, :]
                    full = 9 * (dx + 1) + 3 * (dy + 1) if dx * dy else 3 * (dx + dy + 1)
                    z_up, z_down = z == full + 2.0, z == full + 0.0
                for q in range(5):
                    a = avg_v[q, X - dx, pl.ds(top - dy + 8 * (q % 3), 8), :]
                    terms = (a if hit is None else jnp.where(hit, a, 0.0), jnp.where(z_up, a, 0.0), jnp.where(z_down, a, 0.0))
                    here[q], up[q], down[q] = (
                        new if old is None else old + new for old, new in zip((here[q], up[q], down[q]), terms))
            inv = inv_v[X, pl.ds(top, 8), :]
            for q in range(5):
                edge = at_edges(3 + q // 3, q % 3, X, top)
                total = here[q] + jnp.where(first, edge, roll_lanes(up[q], 1)) + jnp.where(
                    final, edge, roll_lanes(down[q], -1))
                out_ref[q, X - 2, pl.ds(8 * t if isinstance(t, int) else pl.multiple_of(8 * t, 8), 8), :] = total * inv

    def loop(lo, hi, body):
        def step(k, _):
            body(k)
            return _

        lax.fori_loop(lo, hi, step, 0)

    def both_ends(k, low, high):
        return k + low + (k // 2) * (high - low - 2)

    def unpack_y(X, fields):
        for s, near, far in ((0, 7, 6), (1, 40, 41)):
            code[X, near:near + 1, :] = y_recv[s, X, 6:7, :]
            code[X, far:far + 1, :] = y_recv[s, X, 7:8, :]
            if fields:
                for q in range(6):
                    uv[q, X, near:near + 1, :] = y_recv[s, X, q:q + 1, :]

    near_rows = slice(4, 44)
    lane = lanes_of((40, CZ))

    def planes(own, from_lower, from_upper, inner=False):
        lane = lanes_of(own[0].shape)
        ghost = [jnp.where(lane % 2 == 1, roll_lanes(a, 1), roll_lanes(b, -1)) for a, b in zip(from_lower, from_upper)]
        entering, ghost_w, deposits = rim_planes(own, ghost, lane)
        for k, a in enumerate((entering, *ghost_w) if inner else (entering, *ghost_w, *deposits)):
            rim_calc[k, slice(8, 40) if inner else near_rows, :] = a

    def own_signs(X):
        for t in range(4):
            write_signs(X, 8 + 8 * t)

    loop(2, 18, own_signs)
    loop(3, 17, lambda X: count(X, (1, 2, 3)))

    for s in (0, 1):
        @when(has_z[s])
        def _(s=s):
            z_copy(1 - s).wait_recv()
    planes(*([rim[b, 8:40, :] for b in range(3)] for rim in (rim_own, rim_ghost.at[0], rim_ghost.at[1])), inner=True)
    loop(0, 7, lambda k: [weigh(3 + 2 * k + i, (1, 2, 3)) for i in (0, 1)])
    gather(4, 12, 2)

    for s in (0, 1):
        @when(has_y[s])
        def _(s=s):
            y_copies(1 - s, 0)[0].wait_recv()
    for i in (0, 1):
        @when(has_x[i])
        def _(i=i):
            d_copy(i).start()

    def y_ghosts(X):
        unpack_y(X, True)

    loop(2, 18, y_ghosts)

    def ghost_signs(X):
        write_signs(X, 0)
        write_signs(X, 40)

    loop(2, 18, ghost_signs)
    loop(3, 17, lambda X: count(X, (0, 4)))

    for s in (0, 1):
        @when(has_x[s])
        def _(s=s):
            ex_copy(1 - s).wait_recv()
    for i in (0, 1):
        @when(has_y[i])
        def _(i=i):
            ey_copy(i).start()

        @when(has_z[i])
        def _(i=i):
            ez_copy(i, 0).start()

    for s in (0, 1):
        @when(has_y[s])
        def _(s=s):
            y_copies(1 - s, 1)[0].wait_recv()

        for j in (0, 1):
            @when(has_yz[j][s])
            def _(s=s, j=j):
                yz_copy(1 - j, 1 - s).wait_recv()
    planes(*([rim[b, near_rows, :] for b in range(3)] for rim in (rim_own, rim_ghost.at[0], rim_ghost.at[1])))

    loop(0, 7, lambda k: [weigh(3 + 2 * k + i, (0, 4)) for i in (0, 1)])
    for s in (0, 1):
        @when(has_y[s])
        def _(s=s):
            ey_copy(1 - s).wait_recv()
    for i in (0, 1):
        @when(has_z[i])
        def _(i=i):
            ez_copy(i, 1).start()
            ez_copy(i, 2).start()
    loop(0, TILES - 1, lambda k: gather(4, 12, k + k // 2))
    loop(5, 15, scatter)

    for s in (0, 1):
        @when(has_z[s])
        def _(s=s):
            for part in range(3):
                ez_copy(1 - s, part).wait_recv()
    place = lane % SLOT
    at_x = (place < 4) | (place >= 36)

    def with_x(rim, edge):
        low, high = edge[0, near_rows, :], edge[1, near_rows, :]
        return [
            jnp.where(at_x, jnp.where(place < 4, roll_lanes(low, -(32 + 8 * b)), roll_lanes(high, 32 - 8 * b)), rim[b, near_rows, :])
            for b in range(3)
        ]

    planes(with_x(rim_own, edge_own), *(with_x(rim_ghost.at[s], edge_ghost.at[s]) for s in (0, 1)))

    for s in (0, 1):
        @when(has_x[s])
        def _(s=s):
            for copy in x_copies(1 - s):
                copy.wait_recv()
            d_copy(1 - s).wait_recv()

    loop(0, 2, lambda k: unpack_y(1 + 17 * k, True))
    loop(0, 2, lambda k: unpack_y(19 * k, False))

    def end_signs(k):
        for t in range(6):
            write_signs(both_ends(k, 0, 18), 8 * t)

    loop(0, 4, end_signs)
    loop(0, 4, lambda k: count(both_ends(k, 1, 17), range(TILES)))
    loop(0, 4, lambda k: weigh(both_ends(k, 1, 17)))
    loop(0, 2 * TILES, lambda k: gather(1 + 15 * (k // TILES), 3, k % TILES))
    loop(0, 6, lambda k: scatter(2 + k + 10 * (k // 3)))

    for i in (0, 1):
        @when(has_x[i])
        def _(i=i):
            for copy in (*x_copies(i), d_copy(i), ex_copy(i)):
                copy.wait_send()

        @when(has_y[i])
        def _(i=i):
            for copy in (*y_copies(i), ey_copy(i)):
                copy.wait_send()

        @when(has_z[i])
        def _(i=i):
            for copy in (z_copy(i), *(ez_copy(i, part) for part in range(3))):
                copy.wait_send()

        for j in (0, 1):
            @when(has_yz[j][i])
            def _(i=i, j=j):
                yz_copy(j, i).wait_send()


def solution(mesh, nby=NBY, nbz=NBZ):
    nbx = mesh.shape["boxes"] // (nby * nbz)
    f32 = jnp.float32

    def per_device(*args):
        dma = pltpu.SemaphoreType.DMA
        extended = pltpu.VMEM((22, SLAB, CZ), f32)
        values = pltpu.VMEM((6, 22, SLAB, CZ), f32)
        out = pl.pallas_call(
            functools.partial(kernel, (nbx, nby, nbz)),
            out_shape=jax.ShapeDtypeStruct((5, CX, CY, CZ), f32),
            in_specs=[pl.BlockSpec(memory_space=pltpu.HBM)] * 4,
            out_specs=pl.BlockSpec(memory_space=pltpu.VMEM),
            scratch_shapes=[
                values,
                extended, extended, extended, extended, extended, extended,
                pltpu.VMEM((22, SLAB, CZ), jnp.int32),
                pltpu.VMEM((22, SLAB, CZ), jnp.int32),
                pltpu.VMEM((CX, CY, CZ), jnp.int32),
                pltpu.VMEM((CX, CY, CZ), jnp.int32),
                pltpu.VMEM((2, CX, 8, CZ), f32),
                pltpu.VMEM((2, 20, 8, CZ), f32),
                pltpu.VMEM((4, ROWS, CZ), f32),
                pltpu.VMEM((2, 4, ROWS, CZ), f32),
                pltpu.VMEM((CY, CZ), f32),
                pltpu.VMEM((2, ROWS, CZ), f32),
                pltpu.VMEM((2, 2, ROWS, CZ), f32),
                pltpu.VMEM((6, ROWS, CZ), f32),
                values, values, values,
                extended,
                values,
                dma((4,)), dma((2, 2)), dma((2, 2)), dma((2, 2)), dma((2, 2)), dma((2,)), dma((2,)), dma((2,)), dma((2,)),
                dma((2, 2)), dma((2, 2)), dma((2,)), dma((2,)), dma((2,)), dma((2,)), dma((2, 3)), dma((2, 3)),
            ],
            compiler_params=pltpu.CompilerParams(
                collective_id=0, has_side_effects=True, vmem_limit_bytes=38 * 1024 * 1024
            ),
        )(*(pltpu.with_memory_space_constraint(a[0], pltpu.HBM) for a in args))
        return out[None]

    return jax.shard_map(
        per_device,
        mesh=mesh,
        in_specs=(
            P("boxes", None, None, None, None),
            P("boxes", None, None, None),
            P("boxes", None, None, None),
            P("boxes", None, None, None),
        ),
        out_specs=P("boxes", None, None, None, None),
        check_vma=False,
    )
```

```python
import functools

import jax
import jax.numpy as jnp
from jax import lax
from jax.experimental import pallas as pl
from jax.experimental.pallas import tpu as pltpu
from jax.sharding import PartitionSpec as P

NBY = 4
NBZ = 4
CX, CY, CZ = 16, 32, 128
MESH = pl.DeviceIdType.MESH

ROWS = 48
SLAB = 64
SLOT = 40
SIGNS = [(dx, dy) for dx in (-1, 0, 1) for dy in (-1, 0, 1)]


def lanes_of(shape):
    return lax.broadcasted_iota(jnp.int32, shape, len(shape) - 1)


def roll_lanes(a, by):
    return pltpu.roll(a, by % CZ, a.ndim - 1) if by % CZ else a


def roll_rows(a, by):
    return pltpu.roll(a, by % a.shape[0], 0) if by % a.shape[0] else a


def decode(code):
    xy = jnp.floor((code + 0.5) * (1.0 / 3.0))
    x = jnp.floor((code + 0.5) * (1.0 / 9.0))
    return xy, xy - 3.0 * x, code - 3.0 * xy


def towards(xy, y, dx, dy):
    if dy == 0:
        return xy >= 6.0 if dx == 1 else xy <= 2.0
    if dx == 0:
        return y == 1.0 + dy
    return xy == 3.0 * (dx + 1) + (dy + 1)


def moved(a, dx, dy):
    return roll_rows(roll_lanes(a, 2 * dx), dy)


def plane_spread(a, xy, y):
    up = towards(xy, y, 1, 0)
    down = towards(xy, y, -1, 0)

    def along_x(b):
        return b + moved(jnp.where(up, b, 0.0), 1, 0) + moved(jnp.where(down, b, 0.0), -1, 0)

    total = along_x(a)
    for dy in (-1, 1):
        total = total + moved(along_x(jnp.where(towards(xy, y, 0, dy), a, 0.0)), 0, dy)
    return total


def plane_gather(a, xy, y):
    left, right = towards(xy, y, 0, -1), towards(xy, y, 0, 1)

    def along_y(b):
        return b + jnp.where(right, moved(b, 0, -1), jnp.where(left, moved(b, 0, 1), 0.0))

    ahead, behind = along_y(moved(a, -1, 0)), along_y(moved(a, 1, 0))
    chosen = jnp.where(towards(xy, y, 1, 0), ahead, jnp.where(towards(xy, y, -1, 0), behind, 0.0))
    return along_y(a) + chosen


def in_all_slots(a, lane):
    return jnp.where(lane < SLOT, a, jnp.where(lane < 2 * SLOT, roll_lanes(a, SLOT), roll_lanes(a, 2 * SLOT)))


def rim_planes(own, ghost, lane):
    lower = lane % 2 == 1

    def signs(code):
        xy, y, z = decode(code)
        return xy, y, jnp.where(lower, z, 2.0 - z)

    near_own, far_own = signs(own[2]), signs(roll_lanes(own[2], -SLOT))
    near_ghost, far_ghost = signs(ghost[2]), signs(roll_lanes(ghost[2], -SLOT))
    one = jnp.ones(own[0].shape, jnp.float32)

    def spread_ones(plane, sign):
        xy, y, z = plane
        return plane_spread(one if sign == 0 else jnp.where(z == 1.0 + sign, 1.0, 0.0), xy, y)

    entering = spread_ones(near_ghost, 1)
    ghost_count = spread_ones(near_ghost, 0) + spread_ones(far_ghost, 1) + spread_ones(near_own, -1)
    own_count = spread_ones(near_own, 0) + entering + spread_ones(far_own, -1)
    last = lane >= 2 * SLOT

    def weighted(pack, count):
        w = in_all_slots(roll_lanes(pack[1], -2 * SLOT) / count, lane)
        return w * pack[0], w * jnp.where(last, 1.0, pack[1])

    ghost_w = weighted(ghost, ghost_count)
    own_w = weighted(own, own_count)
    xy, y, z = signs(in_all_slots(ghost[2], lane))
    sums = [plane_gather(a + b, xy, y) for a, b in zip(ghost_w, own_w)]
    volume = in_all_slots(roll_lanes(sums[1], -2 * SLOT), lane)
    deposits = [plane_spread(jnp.where(z == 2.0, s / volume, 0.0), xy, y) for s in sums]
    return entering, ghost_w, deposits


TILES = 5


def kernel(
    sizes, u_hbm, vf_hbm, mask_hbm, code_hbm, out_ref,
    uv, code, xy_v, y_v, z_v, xz_v, yz_v, ones_v, total_v, mask_raw, code_raw, y_send, y_recv, rim_own, rim_ghost, edge_send,
    edge_own, edge_ghost, rim_calc, w_v, up_v, down_v, inv_v, avg_v,
    load_sem, x_send_sem, x_recv_sem, y_send_sem, y_recv_sem, d_send_sem, d_recv_sem, z_send_sem, z_recv_sem,
    yz_send_sem, yz_recv_sem, ex_send_sem, ex_recv_sem, ey_send_sem, ey_recv_sem, ez_send_sem, ez_recv_sem,
):
    nbx, nby, nbz = sizes
    me = lax.axis_index("boxes")
    bx, by, bz = me // (nby * nbz), (me // nbz) % nby, me % nbz
    has_x = (bx > 0, bx < nbx - 1)
    has_y = (by > 0, by < nby - 1)
    has_z = (bz > 0, bz < nbz - 1)
    has_yz = [[has_y[j] & has_z[i] for i in (0, 1)] for j in (0, 1)]
    steps = (-1, 1)
    x_step, y_step = nby * nbz, nbz

    def when(cond):
        return pl.when(cond)

    barrier = pltpu.get_barrier_semaphore()
    greeted = 0
    for i in (0, 1):
        met = [(has_x[i], steps[i] * x_step), (has_y[i], steps[i] * y_step), (has_z[i], steps[i])]
        met += [(has_yz[j][i], steps[j] * y_step + steps[i]) for j in (0, 1)]
        for cond, step in met:
            @when(cond)
            def _(step=step):
                pl.semaphore_signal(barrier, inc=1, device_id=(me + step,), device_id_type=MESH)
            greeted = greeted + cond.astype(jnp.int32)

    loads = [
        pltpu.make_async_copy(mask_hbm, mask_raw, load_sem.at[0]),
        pltpu.make_async_copy(code_hbm, code_raw, load_sem.at[1]),
        pltpu.make_async_copy(vf_hbm, uv.at[0, 2:18, 8:40], load_sem.at[2]),
        pltpu.make_async_copy(u_hbm, uv.at[1:6, 2:18, 8:40], load_sem.at[3]),
    ]
    for load in loads:
        load.start()

    def remote(src, dst, send, recv, step):
        return pltpu.make_async_remote_copy(
            src_ref=src, dst_ref=dst, send_sem=send, recv_sem=recv, device_id=(me + step,), device_id_type=MESH)

    def x_copies(i):
        src_u, dst_u = (2, 18) if i == 0 else (17, 1)
        src_c, dst_c = (2, 18) if i == 0 else (16, 0)
        return [
            remote(uv.at[:, src_u, 8:40], uv.at[:, dst_u, 8:40], x_send_sem.at[i, 0], x_recv_sem.at[1 - i, 0],
                   steps[i] * x_step),
            remote(code.at[pl.ds(src_c, 2), 8:40], code.at[pl.ds(dst_c, 2), 8:40], x_send_sem.at[i, 1],
                   x_recv_sem.at[1 - i, 1], steps[i] * x_step),
        ]

    def d_copy(i):
        src, dst = (2, 18) if i == 0 else (16, 0)
        return remote(y_recv.at[:, pl.ds(src, 2)], y_recv.at[:, pl.ds(dst, 2)], d_send_sem.at[i], d_recv_sem.at[1 - i],
                      steps[i] * x_step)

    rim_src, rim_dst = (8, 32), (40, 0)

    def y_copies(i, which=None):
        return [
            remote(y_send.at[i], y_recv.at[1 - i, 2:18], y_send_sem.at[i, 0], y_recv_sem.at[1 - i, 0], steps[i] * y_step),
        ] * (which != 1) + [
            remote(rim_own.at[0:3, pl.ds(rim_src[i], 8)], rim_own.at[0:3, pl.ds(rim_dst[i], 8)], y_send_sem.at[i, 1],
                   y_recv_sem.at[1 - i, 1], steps[i] * y_step),
        ] * (which != 0)

    def z_copy(i):
        return remote(rim_own.at[0:3, 8:40], rim_ghost.at[1 - i, 0:3, 8:40], z_send_sem.at[i], z_recv_sem.at[1 - i], steps[i])

    def yz_copy(j, i):
        return remote(
            rim_own.at[0:3, pl.ds(rim_src[j], 8)], rim_ghost.at[1 - i, 0:3, pl.ds(rim_dst[j], 8)], yz_send_sem.at[j, i],
            yz_recv_sem.at[1 - j, 1 - i], steps[j] * y_step + steps[i])

    def ex_copy(i):
        return remote(edge_send, edge_own.at[1 - i, 8:40], ex_send_sem.at[i], ex_recv_sem.at[1 - i], steps[i] * x_step)

    def ey_copy(i):
        return remote(edge_own.at[:, pl.ds(rim_src[i], 8)], edge_own.at[:, pl.ds(rim_dst[i], 8)], ey_send_sem.at[i],
                      ey_recv_sem.at[1 - i], steps[i] * y_step)

    def ez_copy(i, part):
        rows = pl.ds((8, 0, 40)[part], (32, 8, 8)[part])
        return remote(edge_own.at[:, rows], edge_ghost.at[1 - i, :, rows], ez_send_sem.at[i, part],
                      ez_recv_sem.at[1 - i, part], steps[i])

    loads[0].wait()
    loads[1].wait()

    def write_signs(X, base):
        rows = pl.ds(base, 8)
        c = code[X, rows, :]
        xy, y, z = decode(c)
        xy_v[X, rows, :] = xy
        y_v[X, rows, :] = y
        z_v[X, rows, :] = z
        xz_v[X, rows, :] = xy - y + z
        yz_v[X, rows, :] = 3.0 * y + z
        ones_v[X, rows, :] = jnp.where(z == 2.0, 257, jnp.where(z == 0.0, 65537, 1))

    def own_codes(x, _):
        code[x + 2, 8:40, :] = jnp.where(mask_raw[x] == 1, code_raw[x], 13).astype(jnp.float32)
        return _

    lax.fori_loop(0, CX, own_codes, 0)
    loads[2].wait()
    loads[3].wait()

    def pack_y(x, _):
        for s, near, far in ((0, 8, 9), (1, 39, 38)):
            for q in range(6):
                y_send[s, x, q:q + 1, :] = uv[q, x + 2, near:near + 1, :]
            y_send[s, x, 6:7, :] = code[x + 2, near:near + 1, :]
            y_send[s, x, 7:8, :] = code[x + 2, far:far + 1, :]
        return _

    lax.fori_loop(0, CX, pack_y, 0)
    lane8 = lanes_of((8, CZ))

    def pack_rims(rim, slabs, base):
        blocks = [jnp.zeros((8, CZ), jnp.float32) for _ in range(3)]

        def place(b, value, slot, X):
            lane = slot * SLOT + 2 * X
            blocks[b] = jnp.where(lane8 // 2 == lane // 2, roll_lanes(value, lane + 1), blocks[b])

        for X in slabs:
            near = code[X, pl.ds(base, 8), :]
            place(2, near, 0, X)
            place(2, jnp.where(lane8 == CZ - 1, roll_lanes(near, 1), roll_lanes(near, -1)), 1, X)
            if 1 <= X <= 18:
                for q in range(5):
                    place(q // 3, uv[q + 1, X, pl.ds(base, 8), :], q % 3, X)
                place(1, uv[0, X, pl.ds(base, 8), :], 2, X)
        for b in range(3):
            rim[b, pl.ds(base, 8), :] = blocks[b]

    def pack_own_rims(t, _):
        pack_rims(rim_own, range(2, 18), pl.multiple_of(8 + 8 * t, 8))
        return _

    lax.fori_loop(0, 4, pack_own_rims, 0)

    lane32 = lanes_of((CY, CZ))
    kept = ((lane32 % SLOT) // 4 == 1) | ((lane32 % SLOT) // 4 == 8)
    compact = jnp.zeros((CY, CZ), jnp.float32)
    for b in range(3):
        compact = compact + roll_lanes(jnp.where(kept & (lane32 < (2 if b == 2 else 3) * SLOT), rim_own[b, 8:40, :], 0.0), 8 * b)
    edge_send[...] = compact
    pl.semaphore_wait(barrier, greeted)

    for i in (0, 1):
        @when(has_z[i])
        def _(i=i):
            z_copy(i).start()
    for i in (0, 1):
        @when(has_x[i])
        def _(i=i):
            ex_copy(i).start()
    for i in (0, 1):
        @when(has_y[i])
        def _(i=i):
            for copy in y_copies(i):
                copy.start()

        for j in (0, 1):
            @when(has_yz[j][i])
            def _(i=i, j=j):
                yz_copy(j, i).start()
    for i in (0, 1):
        @when(has_x[i])
        def _(i=i):
            for copy in x_copies(i):
                copy.start()

    tile_row = lax.broadcasted_iota(jnp.int32, (8, CZ), 0)

    def blank_rim(rim, first, rows):
        for b in range(3):
            rim[b, first:first + rows, :] = jnp.full((rows, CZ), 13.0 if b == 2 else 0.0, jnp.float32)

    def blank_edge(rows):
        spot = lanes_of((rows, CZ)) - 16
        is_code = (spot >= 0) & (spot < 2 * SLOT) & (((spot % SLOT) // 4 == 1) | ((spot % SLOT) // 4 == 8))
        return jnp.where(is_code, 13.0, 0.0)

    for s in (0, 1):
        @when(jnp.logical_not(has_y[s]))
        def _(s=s):
            for side in (0, 1):
                edge_own[side, 40 * s:40 * s + 8, :] = blank_edge(8)
            blank_rim(rim_own, 0 if s == 0 else 40, 8)
            for X in range(2, 18):
                y_recv[s, X] = jnp.where(tile_row < 6, 0.0, 13.0)

        @when(jnp.logical_not(has_z[s]))
        def _(s=s):
            blank_rim(rim_ghost.at[s], 8, 32)
            for side in (0, 1):
                edge_ghost[s, side] = blank_edge(ROWS)

        for j in (0, 1):
            @when(jnp.logical_not(has_yz[j][s]))
            def _(s=s, j=j):
                blank_rim(rim_ghost.at[s], 0 if j == 0 else 40, 8)

        @when(jnp.logical_not(has_x[s]))
        def _(s=s):
            u_at, c_at = (1, 0) if s == 0 else (18, 18)
            edge_own[s, 8:40, :] = blank_edge(CY)
            for q in range(6):
                uv[q, u_at, 8:40, :] = jnp.zeros((CY, CZ), jnp.float32)
            for c in (0, 1):
                code[c_at + c, 8:40, :] = jnp.full((CY, CZ), 13.0, jnp.float32)
                for j in (0, 1):
                    y_recv[j, c_at + c] = jnp.where(tile_row < 6, 0.0, 13.0)

    def count(X, tiles):
        for t in tiles:
            top = 7 + 8 * t
            total = ones_v[X, top:top + 8, :]
            for dx, dy in SIGNS:
                if (dx, dy) != (0, 0):
                    at = slice(top - dy, top - dy + 8)
                    signs = (y_v if dx == 0 else xy_v)[X - dx, at, :]
                    total = total + jnp.where(towards(signs, signs, dx, dy), ones_v[X - dx, at, :], 0)
            total_v[X, top:top + 8, :] = total

    first, final = lane8 == 0, lane8 == CZ - 1

    def at_edges(k, slot, X, top):
        shift = CZ * 2 - (slot * SLOT + 2 * X + 1)
        return pltpu.roll(rim_calc[k, pl.ds(top, 8), :], lax.rem(shift, CZ), 1)

    def weigh(X, tiles=range(TILES)):
        for t in tiles:
            top = 7 + 8 * t
            rows = pl.ds(top, 8)
            total = total_v[X, rows, :]
            here = (total & 255).astype(jnp.float32)
            up = ((total >> 8) & 255).astype(jnp.float32)
            down = (total >> 16).astype(jnp.float32)
            edge = at_edges(0, 0, X, top)
            inv = 1.0 / (here + jnp.where(first, edge, roll_lanes(up, 1)) + jnp.where(final, edge, roll_lanes(down, -1)))
            inv_v[X, rows, :] = inv
            w = uv[0, X, rows, :] * inv
            for q in range(6):
                value = w if q == 0 else w * uv[q, X, rows, :]
                k, slot = (2, 2) if q == 0 else (1 + (q - 1) // 3, (q - 1) % 3)
                edge = at_edges(k, slot, X, top)
                w_v[q, X, rows, :] = value
                up_v[q, X, pl.ds(top + 8, 8), :] = value + jnp.where(final, edge, roll_lanes(value, -1))
                down_v[q, X, pl.ds(top + 16, 8), :] = value + jnp.where(first, edge, roll_lanes(value, 1))

    def gather(start, slabs, t):
        top = 7 + 8 * t
        rows = pl.ds(top, 8)

        def step(X, behind, here, ahead):
            targets = []
            for dx, use in ((1, behind), (0, here), (-1, ahead)):
                if use is not None:
                    y, z = y_v[X - dx, rows, :], z_v[X - dx, rows, :]
                    along = None if dx == 0 else towards(xy_v[X - dx, rows, :], None, dx, 0)
                    targets.append((dx, along, y == 2.0, y == 0.0, z == 2.0, z == 0.0))
            new = {dx: [] for dx, *_ in targets}
            for q in range(6):
                lines = [[ref[q, X, pl.ds(top + dy + shift, 8), :] for ref, shift in ((up_v, 8), (down_v, 16), (w_v, 0))] for dy in (-1, 0, 1)]
                for dx, along, y_up, y_down, z_up, z_down in targets:
                    low, mid, high = (jnp.where(z_up, a, jnp.where(z_down, b, c)) for a, b, c in lines)
                    plane = mid + jnp.where(y_up, high, jnp.where(y_down, low, 0.0))
                    if along is not None:
                        plane = jnp.where(along, plane, 0.0)
                    old = {1: behind, 0: here, -1: ahead}[dx][q]
                    new[dx].append(plane if old is None else old + plane)
            return new

        none = [None] * 6
        one = step(start - 1, None, None, none)[-1]
        both = step(start, None, one, none)

        def walk(X, sums):
            new = step(X, list(sums[:6]), list(sums[6:]), none)
            inv = 1.0 / new[1][0]
            for q in range(5):
                avg_v[q, X - 1, pl.ds(top + 8 * (q % 3), 8), :] = new[1][q + 1] * inv
            return (*new[0], *new[-1])

        sums = lax.fori_loop(
            0, slabs // 2, lambda k, sums: walk(start + 2 + 2 * k, walk(start + 1 + 2 * k, sums)), (*both[0], *both[-1]))
        if slabs % 2:
            walk(start + slabs, sums)

    def scatter(X, tiles=range(4)):
        for t in tiles:
            top = 8 + 8 * t
            here, up, down = [None] * 5, [None] * 5, [None] * 5
            for dx, dy in SIGNS:
                at = pl.ds(top - dy, 8)
                if (dx, dy) == (0, 0):
                    z = z_v[X, at, :]
                    hit, z_up, z_down = None, z == 2.0, z == 0.0
                else:
                    signs = (y_v if dx == 0 else xy_v)[X - dx, at, :]
                    hit = towards(signs, signs, dx, dy)
                    z = (code if dx * dy else yz_v if dx == 0 else xz_v)[X - dx, at, :]
                    full = 9 * (dx + 1) + 3 * (dy + 1) if dx * dy else 3 * (dx + dy + 1)
                    z_up, z_down = z == full + 2.0, z == full + 0.0
                for q in range(5):
                    a = avg_v[q, X - dx, pl.ds(top - dy + 8 * (q % 3), 8), :]
                    terms = (a if hit is None else jnp.where(hit, a, 0.0), jnp.where(z_up, a, 0.0), jnp.where(z_down, a, 0.0))
                    here[q], up[q], down[q] = (
                        new if old is None else old + new for old, new in zip((here[q], up[q], down[q]), terms))
            inv = inv_v[X, pl.ds(top, 8), :]
            for q in range(5):
                edge = at_edges(3 + q // 3, q % 3, X, top)
                total = here[q] + jnp.where(first, edge, roll_lanes(up[q], 1)) + jnp.where(
                    final, edge, roll_lanes(down[q], -1))
                out_ref[q, X - 2, pl.ds(8 * t if isinstance(t, int) else pl.multiple_of(8 * t, 8), 8), :] = total * inv

    def loop(lo, hi, body):
        def step(k, _):
            body(k)
            return _

        lax.fori_loop(lo, hi, step, 0)

    def both_ends(k, low, high):
        return k + low + (k // 2) * (high - low - 2)

    def unpack_y(X, fields):
        for s, near, far in ((0, 7, 6), (1, 40, 41)):
            code[X, near:near + 1, :] = y_recv[s, X, 6:7, :]
            code[X, far:far + 1, :] = y_recv[s, X, 7:8, :]
            if fields:
                for q in range(6):
                    uv[q, X, near:near + 1, :] = y_recv[s, X, q:q + 1, :]

    near_rows = slice(4, 44)
    lane = lanes_of((40, CZ))

    def planes(own, from_lower, from_upper, inner=False):
        lane = lanes_of(own[0].shape)
        ghost = [jnp.where(lane % 2 == 1, roll_lanes(a, 1), roll_lanes(b, -1)) for a, b in zip(from_lower, from_upper)]
        entering, ghost_w, deposits = rim_planes(own, ghost, lane)
        for k, a in enumerate((entering, *ghost_w) if inner else (entering, *ghost_w, *deposits)):
            rim_calc[k, slice(8, 40) if inner else near_rows, :] = a

    def own_signs(X):
        for t in range(4):
            write_signs(X, 8 + 8 * t)

    loop(2, 18, own_signs)
    loop(3, 17, lambda X: count(X, (1, 2, 3)))

    for s in (0, 1):
        @when(has_z[s])
        def _(s=s):
            z_copy(1 - s).wait_recv()
    planes(*([rim[b, 8:40, :] for b in range(3)] for rim in (rim_own, rim_ghost.at[0], rim_ghost.at[1])), inner=True)
    loop(0, 7, lambda k: [weigh(3 + 2 * k + i, (1, 2, 3)) for i in (0, 1)])
    gather(4, 12, 2)

    for s in (0, 1):
        @when(has_y[s])
        def _(s=s):
            y_copies(1 - s, 0)[0].wait_recv()
    for i in (0, 1):
        @when(has_x[i])
        def _(i=i):
            d_copy(i).start()

    def y_ghosts(X):
        unpack_y(X, True)

    loop(2, 18, y_ghosts)

    def ghost_signs(X):
        write_signs(X, 0)
        write_signs(X, 40)

    loop(2, 18, ghost_signs)
    loop(3, 17, lambda X: count(X, (0, 4)))

    for s in (0, 1):
        @when(has_x[s])
        def _(s=s):
            ex_copy(1 - s).wait_recv()
    for i in (0, 1):
        @when(has_y[i])
        def _(i=i):
            ey_copy(i).start()

        @when(has_z[i])
        def _(i=i):
            ez_copy(i, 0).start()

    for s in (0, 1):
        @when(has_y[s])
        def _(s=s):
            y_copies(1 - s, 1)[0].wait_recv()

        for j in (0, 1):
            @when(has_yz[j][s])
            def _(s=s, j=j):
                yz_copy(1 - j, 1 - s).wait_recv()
    planes(*([rim[b, near_rows, :] for b in range(3)] for rim in (rim_own, rim_ghost.at[0], rim_ghost.at[1])))

    loop(0, 7, lambda k: [weigh(3 + 2 * k + i, (0, 4)) for i in (0, 1)])
    for s in (0, 1):
        @when(has_y[s])
        def _(s=s):
            ey_copy(1 - s).wait_recv()
    for i in (0, 1):
        @when(has_z[i])
        def _(i=i):
            ez_copy(i, 1).start()
            ez_copy(i, 2).start()
    loop(0, TILES - 1, lambda k: gather(4, 12, k + k // 2))
    loop(5, 15, scatter)

    for s in (0, 1):
        @when(has_z[s])
        def _(s=s):
            for part in range(3):
                ez_copy(1 - s, part).wait_recv()
    place = lane % SLOT
    at_x = (place < 4) | (place >= 36)

    def with_x(rim, edge):
        low, high = edge[0, near_rows, :], edge[1, near_rows, :]
        return [
            jnp.where(at_x, jnp.where(place < 4, roll_lanes(low, -(32 + 8 * b)), roll_lanes(high, 32 - 8 * b)), rim[b, near_rows, :])
            for b in range(3)
        ]

    planes(with_x(rim_own, edge_own), *(with_x(rim_ghost.at[s], edge_ghost.at[s]) for s in (0, 1)))

    for s in (0, 1):
        @when(has_x[s])
        def _(s=s):
            for copy in x_copies(1 - s):
                copy.wait_recv()
            d_copy(1 - s).wait_recv()

    loop(0, 2, lambda k: unpack_y(1 + 17 * k, True))
    loop(0, 2, lambda k: unpack_y(19 * k, False))

    def end_signs(k):
        for t in range(6):
            write_signs(both_ends(k, 0, 18), 8 * t)

    loop(0, 4, end_signs)
    loop(0, 4, lambda k: count(both_ends(k, 1, 17), range(TILES)))
    loop(0, 4, lambda k: weigh(both_ends(k, 1, 17)))
    loop(0, 2 * TILES, lambda k: gather(1 + 15 * (k // TILES), 3, k % TILES))
    loop(0, 6, lambda k: scatter(2 + k + 10 * (k // 3)))

    for i in (0, 1):
        @when(has_x[i])
        def _(i=i):
            for copy in (*x_copies(i), d_copy(i), ex_copy(i)):
                copy.wait_send()

        @when(has_y[i])
        def _(i=i):
            for copy in (*y_copies(i), ey_copy(i)):
                copy.wait_send()

        @when(has_z[i])
        def _(i=i):
            for copy in (z_copy(i), *(ez_copy(i, part) for part in range(3))):
                copy.wait_send()

        for j in (0, 1):
            @when(has_yz[j][i])
            def _(i=i, j=j):
                yz_copy(j, i).wait_send()


def solution(mesh, nby=NBY, nbz=NBZ):
    nbx = mesh.shape["boxes"] // (nby * nbz)
    f32 = jnp.float32

    def per_device(*args):
        dma = pltpu.SemaphoreType.DMA
        extended = pltpu.VMEM((22, SLAB, CZ), f32)
        values = pltpu.VMEM((6, 22, SLAB, CZ), f32)
        out = pl.pallas_call(
            functools.partial(kernel, (nbx, nby, nbz)),
            out_shape=jax.ShapeDtypeStruct((5, CX, CY, CZ), f32),
            in_specs=[pl.BlockSpec(memory_space=pltpu.HBM)] * 4,
            out_specs=pl.BlockSpec(memory_space=pltpu.VMEM),
            scratch_shapes=[
                values,
                extended, extended, extended, extended, extended, extended,
                pltpu.VMEM((22, SLAB, CZ), jnp.int32),
                pltpu.VMEM((22, SLAB, CZ), jnp.int32),
                pltpu.VMEM((CX, CY, CZ), jnp.int32),
                pltpu.VMEM((CX, CY, CZ), jnp.int32),
                pltpu.VMEM((2, CX, 8, CZ), f32),
                pltpu.VMEM((2, 20, 8, CZ), f32),
                pltpu.VMEM((4, ROWS, CZ), f32),
                pltpu.VMEM((2, 4, ROWS, CZ), f32),
                pltpu.VMEM((CY, CZ), f32),
                pltpu.VMEM((2, ROWS, CZ), f32),
                pltpu.VMEM((2, 2, ROWS, CZ), f32),
                pltpu.VMEM((6, ROWS, CZ), f32),
                values, values, values,
                extended,
                values,
                dma((4,)), dma((2, 2)), dma((2, 2)), dma((2, 2)), dma((2, 2)), dma((2,)), dma((2,)), dma((2,)), dma((2,)),
                dma((2, 2)), dma((2, 2)), dma((2,)), dma((2,)), dma((2,)), dma((2,)), dma((2, 3)), dma((2, 3)),
            ],
            compiler_params=pltpu.CompilerParams(
                collective_id=0, has_side_effects=True, vmem_limit_bytes=38 * 1024 * 1024
            ),
        )(*(pltpu.with_memory_space_constraint(a[0], pltpu.HBM) for a in args))
        return out[None]

    return jax.shard_map(
        per_device,
        mesh=mesh,
        in_specs=(
            P("boxes", None, None, None, None),
            P("boxes", None, None, None),
            P("boxes", None, None, None),
            P("boxes", None, None, None),
        ),
        out_specs=P("boxes", None, None, None, None),
        check_vma=False,
    )
```
